32 devices in a mesh: grp: 2 (over y), row: 16 (over z, x, core).
Axes of the slice: x: 2, y: 2, z: 4, core: 2. Of those that a mesh axis runs over, the one named last changes fastest.
Arguments:
- cells: float32 [256, 128, 192], P(('grp', 'row')), parts along dimension 0, may hold values from -6 to 6
- n_train: int32 [2], P('grp'), parts along dimension 0, may hold values from 16 to 127
- present: int32 [256], P('grp'), parts along dimension 0, may hold values from 0 to 1, as said below
- norm_gain: float32 [3, 192], replicated, may hold values from 0.1 to 1.9
- feat_qkv: bfloat16 [3, 192, 192], replicated, may hold values from -6 to 6
- feat_out: bfloat16 [192, 192], replicated, may hold values from -0.4375 to 0.4375
- item_qkv: bfloat16 [3, 192, 192], replicated, may hold values from -6 to 6
- item_out: bfloat16 [192, 192], replicated, may hold values from -0.875 to 0.875
- mlp_in: bfloat16 [192, 768], replicated, may hold values from -0.4375 to 0.4375
- mlp_out: bfloat16 [768, 192], replicated, may hold values from -0.21875 to 0.21875
Outputs:
- result: float32 [256, 128, 192], P(('grp', 'row')), parts along dimension 0
The draws below stay inside these ranges and needn't reach their ends.
There are 2 independent parts, one for each index of `grp`. The reference program is written for one: setup_inputs(seed, part) draws one part's arguments, and reference() takes and returns one part's arrays. A program takes and returns all parts, laid end to end along the dimension named above; an argument that names none is the same for every part. Nothing has to cross between parts.
Inputs may be any that keep to these rules, and one draw needn't show every extreme that they name: At least one of the 128 features is present.
All inputs are finite; a program needn't handle non-finite values.
Results may differ from the reference program's by a relative error of at most 0.03.
The reference program's roundings to bfloat16 on the way count: a program that leaves them out, or rounds other values in their place, can miss the bound.
Values may be sent and summed in bfloat16 or wider, within the bound.
A program may use at most 64 MiB of HBM per device.

```python
import math
import jax
import jax.numpy as jnp
from jax import lax

E = 192
HEADS = 6
FF = 768
FEAT = 128
ROWS = 128


def drawn_triplet(key):
    base = jax.random.normal(key, (3, E, E), jnp.float32) / math.sqrt(E)
    stacked = jnp.stack([3.0 * base[0], 3.0 * base[1], base[2]])
    return jnp.clip(stacked, -6.0, 6.0).astype(jnp.bfloat16)


def draw_feat_qkv(key, part):
    return drawn_triplet(jax.random.fold_in(key, 11))


def draw_item_qkv(key, part):
    return drawn_triplet(jax.random.fold_in(key, 23))


def draw_present(key, part):
    levels = jax.random.randint(jax.random.fold_in(key, 5), (FEAT,), 0, 4)
    forced = jax.random.randint(jax.random.fold_in(key, 6), (), 0, FEAT)
    position = jnp.arange(FEAT, dtype=jnp.int32)
    return jnp.where((levels > 0) | (position == forced), 1, 0).astype(jnp.int32)


def block_levels(rng, dims, cuts, smallest, high):
    def one(dim, blocks):
        draws = jax.random.uniform(jax.random.fold_in(jax.random.fold_in(rng, 6), dim), (blocks,), jnp.float32, smallest / len(cuts), high / len(cuts))
        return jnp.repeat(jnp.exp(draws), dims[dim] // blocks).reshape((-1,) + (1,) * (len(dims) - dim - 1))

    loudness = one(*cuts[0])
    for cut in cuts[1:]:
        loudness = loudness * one(*cut)
    return loudness


def bell_draw(key, dims, width, bound, pieces=(), kind=jnp.bfloat16):
    values = jax.random.normal(key, dims, jnp.float32) * width
    if len(pieces) > 0:
        values = block_levels(key, dims, pieces, -0.22, 0.18) * values
    return jnp.clip(values, min=-bound, max=bound).astype(kind)


def setup_inputs(seed: int = 0, part: int = 0) -> dict:
    splits = jax.random.split(jax.random.key(seed), 11)
    own_keys = jax.random.split(jax.random.fold_in(splits[10], part), 11)
    return {
        "cells": bell_draw(own_keys[0], (ROWS, FEAT, E), 1.0, 6.0, ((0, 16),), jnp.float32),
        "n_train": jax.random.randint(own_keys[1], (1,), ROWS // 8, ROWS).astype(jnp.int32),
        "present": draw_present(jax.random.fold_in(jax.random.fold_in(splits[10], part), 71), part),
        "norm_gain": jnp.clip(1.0 + 0.18 * jax.random.normal(splits[3], (3, E), jnp.float32), 0.1, 1.9),
        "feat_qkv": draw_feat_qkv(jax.random.fold_in(splits[10], 71), part),
        "feat_out": bell_draw(splits[5], (E, E), E ** -0.5, 0.4375),
        "item_qkv": draw_item_qkv(jax.random.fold_in(splits[10], 71), part),
        "item_out": bell_draw(splits[7], (E, E), (E // 4) ** -0.5, 0.875),
        "mlp_in": bell_draw(splits[8], (E, FF), E ** -0.5, 0.4375),
        "mlp_out": bell_draw(splits[9], (FF, E), FF ** -0.5, 0.21875),
    }


norm_floor = 0.25
masked_score = -1e+30

def widen(array):
    return array.astype(jnp.float32)

def layer_norm(stream, gain):
    average = lax.optimization_barrier(jnp.mean(stream, axis=-1, keepdims=True))
    centred = stream - average
    spread = lax.optimization_barrier(jnp.mean(centred * centred, axis=-1, keepdims=True))
    return centred * lax.rsqrt(spread + norm_floor) * gain

def softmax_rows(scores):
    largest = lax.optimization_barrier(jnp.max(scores, axis=-1, keepdims=True))
    exponent = jnp.exp(scores - largest)
    return exponent / lax.optimization_barrier(jnp.sum(exponent, axis=-1, keepdims=True))

def reference(cells, n_train, present, norm_gain, feat_qkv, feat_out, item_qkv, item_out, mlp_in, mlp_out):
    head_size = E // HEADS
    scale = 1.0 / math.sqrt(head_size)
    row_group = math.gcd(ROWS, 128)
    query_rows = min(512, ROWS)
    highest = lax.Precision.HIGHEST

    def feature_group(stream):
        normed = layer_norm(stream, norm_gain[0]).astype(jnp.bfloat16)
        triplet = jnp.einsum('rfe,ced->crfd', widen(normed), widen(feat_qkv))
        triplet = triplet.reshape(3, row_group, FEAT, HEADS, head_size)
        values = widen(triplet[2].astype(jnp.bfloat16))
        scores = jnp.einsum('rfhd,rghd->rhfg', triplet[0], triplet[1], precision=highest) * scale
        scores = jnp.where(present[None, None, None, :] > 0, scores, masked_score)
        weights = softmax_rows(scores).astype(jnp.bfloat16)
        context = jnp.einsum('rhfg,rghd->rfhd', widen(weights), values).astype(jnp.bfloat16)
        context = context.reshape(row_group, FEAT, E)
        return stream + jnp.dot(context, feat_out, preferred_element_type=jnp.float32)
    cells_mid = lax.map(feature_group, cells.reshape(ROWS // row_group, row_group, FEAT, E)).reshape(ROWS, FEAT, E)
    key_live = jnp.arange(ROWS, dtype=jnp.int32) < n_train[0]

    def item_feature(stream):
        normed = layer_norm(stream, norm_gain[1]).astype(jnp.bfloat16)
        triplet = jnp.einsum('re,ced->crd', widen(normed), widen(item_qkv))
        keys = triplet[1].reshape(ROWS, HEADS, head_size)
        values = widen(triplet[2].astype(jnp.bfloat16)).reshape(ROWS, HEADS, head_size)
        queries = triplet[0].reshape(ROWS // query_rows, query_rows, HEADS, head_size)

        def query_group(chosen):
            scores = jnp.einsum('qhd,shd->hqs', chosen, keys, precision=highest) * scale
            scores = jnp.where(key_live[None, None, :], scores, masked_score)
            weights = softmax_rows(scores).astype(jnp.bfloat16)
            return jnp.einsum('hqs,shd->qhd', widen(weights), values).astype(jnp.bfloat16)
        context = lax.map(query_group, queries).reshape(ROWS, E)
        late = stream + jnp.dot(context, item_out, preferred_element_type=jnp.float32)
        normed_late = layer_norm(late, norm_gain[2]).astype(jnp.bfloat16)
        hidden = jax.nn.gelu(jnp.dot(normed_late, mlp_in, preferred_element_type=jnp.float32), approximate=False).astype(jnp.bfloat16)
        return late + jnp.dot(hidden, mlp_out, preferred_element_type=jnp.float32)
    updated = lax.map(item_feature, jnp.transpose(cells_mid, (1, 0, 2)))
    return jnp.transpose(updated, (1, 0, 2))
```

```python
import functools
import math

import jax
import jax.numpy as jnp
from jax import lax
from jax.experimental import pallas as pl
from jax.experimental.pallas import tpu as pltpu
from jax.sharding import PartitionSpec as P

HEADS = 6
LANES = 128
SUBLANES = 8


norm_floor = 0.25
masked_score = -1e30


def layer_norm(stream, gain):
    average = jnp.mean(stream, axis=-1, keepdims=True)
    centred = stream - average
    spread = jnp.mean(centred * centred, axis=-1, keepdims=True)
    return centred * lax.rsqrt(spread + norm_floor) * gain


def softmax_rows(scores):
    largest = jnp.max(scores, axis=-1, keepdims=True)
    exponent = jnp.exp(scores - largest)
    return exponent / jnp.sum(exponent, axis=-1, keepdims=True)


def plain_body(
    cells, n_train, present, norm_gain, feat_qkv, feat_out, item_qkv, item_out, mlp_in, mlp_out
):
    row_dev, feature_count, model_width = cells.shape
    devices_row = lax.axis_size("row")
    total_rows = row_dev * devices_row
    feat_dev = feature_count // devices_row
    head_size = model_width // HEADS
    scale = 1.0 / math.sqrt(head_size)
    query_rows = min(512, total_rows)
    highest = lax.Precision.HIGHEST
    normed = layer_norm(cells, norm_gain[0]).astype(jnp.bfloat16)
    triplet = jnp.einsum("rfe,ced->crfd", normed, feat_qkv, preferred_element_type=jnp.float32)
    triplet = triplet.reshape(3, row_dev, feature_count, HEADS, head_size)
    feat_values = triplet[2].astype(jnp.bfloat16)
    scores = jnp.einsum("rfhd,rghd->rhfg", triplet[0], triplet[1], precision=highest) * scale
    scores = jnp.where(present[None, None, None, :] > 0, scores, masked_score)
    weights = softmax_rows(scores).astype(jnp.bfloat16)
    context = jnp.einsum(
        "rhfg,rghd->rfhd", weights, feat_values, preferred_element_type=jnp.float32
    ).astype(jnp.bfloat16)
    context = context.reshape(row_dev, feature_count, model_width)
    cells_mid = cells + jnp.dot(context, feat_out, preferred_element_type=jnp.float32)
    key_live = lax.iota(jnp.int32, total_rows) < n_train[0]
    arrived = lax.all_to_all(
        cells_mid.reshape(row_dev, devices_row, feat_dev, model_width).astype(jnp.bfloat16),
        "row",
        split_axis=1,
        concat_axis=0,
        tiled=True,
    ).astype(jnp.float32)
    members = arrived.shape[2]
    stream = arrived.reshape(total_rows, members, model_width)
    normed_rows = layer_norm(stream, norm_gain[1]).astype(jnp.bfloat16)
    triples = jnp.einsum("rke,ced->kcrd", normed_rows, item_qkv, preferred_element_type=jnp.float32)

    def one_feature(triple):
        keys = triple[1].reshape(total_rows, HEADS, head_size)
        values = triple[2].astype(jnp.bfloat16).reshape(total_rows, HEADS, head_size)
        queries = triple[0].reshape(total_rows // query_rows, query_rows, HEADS, head_size)

        def query_group(chosen):
            group_scores = jnp.einsum("qhd,shd->hqs", chosen, keys, precision=highest) * scale
            group_scores = jnp.where(key_live[None, None, :], group_scores, masked_score)
            group_weights = softmax_rows(group_scores).astype(jnp.bfloat16)
            return jnp.einsum(
                "hqs,shd->qhd", group_weights, values, preferred_element_type=jnp.float32
            ).astype(jnp.bfloat16)

        return lax.map(query_group, queries).reshape(total_rows, model_width)

    gathered = lax.map(one_feature, triples)
    late = stream + jnp.dot(
        jnp.transpose(gathered, (1, 0, 2)), item_out, preferred_element_type=jnp.float32
    )
    normed_late = layer_norm(late, norm_gain[2]).astype(jnp.bfloat16)
    hidden = jax.nn.gelu(
        jnp.dot(normed_late, mlp_in, preferred_element_type=jnp.float32), approximate=False
    ).astype(jnp.bfloat16)
    updated = late + jnp.dot(hidden, mlp_out, preferred_element_type=jnp.float32)
    returned = lax.all_to_all(
        updated.reshape(total_rows, 1, members, model_width).astype(jnp.bfloat16),
        "row",
        split_axis=0,
        concat_axis=1,
        tiled=True,
    ).astype(jnp.float32)
    return returned.reshape(row_dev, feature_count, model_width)


def matmul(left, right, dims=(1, 0)):
    return lax.dot_general(
        left, right, (((dims[0],), (dims[1],)), ((), ())), preferred_element_type=jnp.float32
    )


def identity(size):
    down = lax.broadcasted_iota(jnp.int32, (size, size), 0)
    across = lax.broadcasted_iota(jnp.int32, (size, size), 1)
    return jnp.where(down == across, 1.0, 0.0).astype(jnp.bfloat16)


def prepare_weights(qkv_ref, turned_ref, spread_ref):
    width = qkv_ref.shape[1]
    head = width // HEADS
    eye = identity(width)
    turned_ref[:width, :] = matmul(eye, qkv_ref[0], (1, 1)).astype(jnp.bfloat16)
    turned_ref[width:, :] = matmul(eye, qkv_ref[2], (1, 1)).astype(jnp.bfloat16)
    down = lax.broadcasted_iota(jnp.int32, (width, 4 * width), 0)
    across = lax.broadcasted_iota(jnp.int32, (width, 4 * width), 1)
    source = (across // (4 * head)) * head + across % head
    pick = jnp.where(down == source, 1.0, 0.0).astype(jnp.bfloat16)
    spread_ref[...] = matmul(qkv_ref[1], pick).astype(jnp.bfloat16)


def attention(normed, turned_ref, spread_ref, bias_ref):
    tokens, width = normed.shape
    size = bias_ref.shape[0]
    head = width // HEADS
    wide = 4 * head
    turned = matmul(turned_ref[...], normed, (1, 1))
    keys = matmul(normed, spread_ref[...])
    queries = turned[:width] * (math.log2(math.e) / math.sqrt(head))
    query_high = queries.astype(jnp.bfloat16)
    query_low = (queries - query_high.astype(jnp.float32)).astype(jnp.bfloat16)
    values = turned[width:].astype(jnp.bfloat16)
    lane = lax.broadcasted_iota(jnp.int32, (1, 4 * width), 1)
    rounded = keys.astype(jnp.bfloat16).astype(jnp.float32)
    keys = jnp.where(lane % wide < 2 * head, keys, keys - rounded).astype(jnp.bfloat16)
    blocks = []
    for block in range(tokens // size):
        here = slice(block * size, (block + 1) * size)
        contexts = []
        for h in range(HEADS):
            rows = slice(h * head, (h + 1) * head)
            high, low = query_high[rows, here], query_low[rows, here]
            query = jnp.concatenate([high, low, high, low], axis=0)
            scores = matmul(keys[here, h * wide : (h + 1) * wide], query) + bias_ref[...]
            exponent = jnp.exp2(scores - jnp.max(scores, axis=0, keepdims=True))
            share = 1.0 / jnp.sum(exponent, axis=0, keepdims=True)
            weights = (exponent * share).astype(jnp.bfloat16)
            contexts.append(matmul(values[rows, here], weights))
        blocks.append(jnp.concatenate(contexts, axis=0))
    return blocks


def kernel(
    devices,
    n_train_ref, cells_ref, present_ref, gain_ref, feat_qkv_ref, feat_out_ref, item_qkv_ref,
    item_out_ref, mlp_in_ref, mlp_out_ref,
    out_ref,
    turned_f, spread_f, turned_i, spread_i, bias_f, bias_i, mid_a, mid_b, mid, send, recv, back,
    home, send_sem, recv_sem, back_sem, home_sem,
):
    me = lax.axis_index("row")
    rows, feats, width = cells_ref.shape
    feat_dev = feats // devices
    pairs = feat_dev // 2
    total_rows = rows * devices
    block = 2 * rows
    group = devices * block
    rest = width - LANES

    barrier = pltpu.get_barrier_semaphore()

    def greet(step, carry):
        pl.semaphore_signal(
            barrier, inc=1, device_id={"row": lax.rem(me + step, devices)},
            device_id_type=pl.DeviceIdType.MESH,
        )
        return carry

    lax.fori_loop(1, devices, greet, 0)

    prepare_weights(feat_qkv_ref, turned_f, spread_f)
    prepare_weights(item_qkv_ref, turned_i, spread_i)
    live = jnp.where(present_ref[...] > 0, 0.0, masked_score)
    bias_f[...] = jnp.broadcast_to(live, (feats, feats)).T
    number = lax.broadcasted_iota(jnp.int32, (total_rows, total_rows), 0)
    bias_i[...] = jnp.where(number < n_train_ref[0], 0.0, masked_score)

    def feature_rows(step, carry):
        cells = cells_ref[pl.ds(step * 2, 2)].reshape(2 * feats, width)
        normed = layer_norm(cells, gain_ref[0:1, :]).astype(jnp.bfloat16)
        contexts = attention(normed, turned_f, spread_f, bias_f)
        context = jnp.concatenate(contexts, axis=1).astype(jnp.bfloat16)
        updated = cells + matmul(context, feat_out_ref[...], (0, 0))
        here = pl.ds(pl.multiple_of(step * 2 * feats, 2 * feats), 2 * feats)
        mid_a[here, :] = updated[:, :LANES]
        mid_b[here, :rest] = updated[:, LANES:]
        return carry

    lax.fori_loop(0, rows // 2, feature_rows, 0)

    def outgoing(pair, step):
        to = lax.rem(me + step, devices)
        return pltpu.make_async_remote_copy(
            src_ref=send.at[pair, to], dst_ref=recv.at[pair, me],
            send_sem=send_sem.at[pair, step], recv_sem=recv_sem.at[pair, step],
            device_id={"row": to}, device_id_type=pl.DeviceIdType.MESH,
        )

    def returning(pair, step):
        to = lax.rem(me + step, devices)
        return pltpu.make_async_remote_copy(
            src_ref=back.at[pair, to], dst_ref=home.at[pair, me],
            send_sem=back_sem.at[pair, step], recv_sem=home_sem.at[pair, step],
            device_id={"row": to}, device_id_type=pl.DeviceIdType.MESH,
        )

    def each(act):
        def one(step, carry):
            act(step)
            return carry

        lax.fori_loop(1, devices, one, 0)

    pl.semaphore_wait(barrier, devices - 1)

    for pair in range(pairs):
        firsts, lasts = [], []
        for owner in range(devices):
            for one in range(2):
                take = pl.ds(owner * feat_dev + pair * 2 + one, rows, stride=feats)
                firsts.append(mid_a[take, :])
                lasts.append(mid_b[take, :])
        stream = jnp.concatenate(
            [jnp.concatenate(firsts, axis=0), jnp.concatenate(lasts, axis=0)[:, :rest]], axis=1
        )
        mid[pair] = stream
        normed = layer_norm(stream, gain_ref[1:2, :]).astype(jnp.bfloat16)
        send[pair] = normed.reshape(devices, block, width)
        recv[pair, me] = send[pair, me]
        each(lambda step: outgoing(pair, step).start())

    def item_pair(pair, carry):
        each(lambda step: outgoing(pair, step).wait_recv())
        arrived = recv[pair].astype(jnp.float32).reshape(devices, 2, rows, width)
        normed = jnp.concatenate(
            [arrived[:, one].reshape(total_rows, width) for one in range(2)], axis=0
        ).astype(jnp.bfloat16)
        contexts = attention(normed, turned_i, spread_i, bias_i)
        turned = [context.T.reshape(devices, 1, rows, width) for context in contexts]
        context = jnp.concatenate(turned, axis=1).reshape(devices, block, width)
        back[pair] = context.astype(jnp.bfloat16)
        home[pair, me] = back[pair, me]
        each(lambda step: returning(pair, step).start())
        return carry

    lax.fori_loop(0, pairs, item_pair, 0)

    def finish(pair, carry):
        each(lambda step: returning(pair, step).wait_recv())
        context = home[pair].reshape(group, width)
        late = mid[pair] + matmul(context, item_out_ref[...])
        normed = layer_norm(late, gain_ref[2:3, :]).astype(jnp.bfloat16)
        inner = matmul(normed, mlp_in_ref[...])
        hidden = (0.5 * inner * (1.0 + lax.erf(inner * math.sqrt(0.5)))).astype(jnp.bfloat16)
        done = late + matmul(hidden, mlp_out_ref[...])
        for owner in range(devices):
            for one in range(2):
                start = (owner * 2 + one) * rows
                put = pl.ds(owner * feat_dev + pair * 2 + one, rows, stride=feats)
                mid_a[put, :] = done[start : start + rows, :LANES]
                mid_b[put, :rest] = done[start : start + rows, LANES:]
        return carry

    lax.fori_loop(0, pairs, finish, 0)
    for row in range(rows):
        out_ref[row, :, :LANES] = mid_a[row * feats : (row + 1) * feats, :]
        out_ref[row, :, LANES:] = mid_b[row * feats : (row + 1) * feats, :rest]

    for pair in range(pairs):
        each(lambda step: outgoing(pair, step).wait_send())
        each(lambda step: returning(pair, step).wait_send())


def body(
    cells, n_train, present, norm_gain, feat_qkv, feat_out, item_qkv, item_out, mlp_in, mlp_out
):
    devices = lax.axis_size("row")
    rows, feats, width = cells.shape
    feat_dev = feats // devices
    fits = rows == SUBLANES and feat_dev % 2 == 0 and LANES < width <= 2 * LANES
    fits = fits and rows * devices == LANES and feats == LANES and width % (HEADS * 16) == 0
    if not fits:
        return plain_body(
            cells, n_train, present, norm_gain, feat_qkv, feat_out, item_qkv, item_out, mlp_in,
            mlp_out,
        )
    total_rows = rows * devices
    pairs = feat_dev // 2
    vmem = pl.BlockSpec(memory_space=pltpu.VMEM)
    bf16, f32 = jnp.bfloat16, jnp.float32
    slots = pltpu.VMEM((pairs, devices, 2 * rows, width), bf16)
    sems = pltpu.SemaphoreType.DMA((pairs, devices))
    return pl.pallas_call(
        functools.partial(kernel, devices),
        out_shape=jax.ShapeDtypeStruct(cells.shape, f32),
        in_specs=[pl.BlockSpec(memory_space=pltpu.SMEM)] + [vmem] * 9,
        out_specs=vmem,
        scratch_shapes=[
            pltpu.VMEM((2 * width, width), bf16),
            pltpu.VMEM((width, 4 * width), bf16),
            pltpu.VMEM((2 * width, width), bf16),
            pltpu.VMEM((width, 4 * width), bf16),
            pltpu.VMEM((feats, feats), f32),
            pltpu.VMEM((total_rows, total_rows), f32),
            pltpu.VMEM((rows * feats, LANES), f32),
            pltpu.VMEM((rows * feats, LANES), f32),
            pltpu.VMEM((pairs, 2 * total_rows, width), f32),
            slots, slots, slots, slots, sems, sems, sems, sems,
        ],
        compiler_params=pltpu.CompilerParams(
            collective_id=0, has_side_effects=True, vmem_limit_bytes=48 * 1024 * 1024
        ),
    )(
        n_train, cells, present.reshape(1, feats), norm_gain, feat_qkv, feat_out, item_qkv, item_out,
        mlp_in, mlp_out,
    )


def solution(mesh):
    return jax.shard_map(
        body,
        mesh=mesh,
        in_specs=(
            P(("grp", "row"), None, None),
            P("grp"),
            P("grp"),
            P(),
            P(),
            P(),
            P(),
            P(),
            P(),
            P(),
        ),
        out_specs=P(("grp", "row"), None, None),
        check_vma=False,
    )
```

```python
import functools
import math

import jax
import jax.numpy as jnp
from jax import lax
from jax.experimental import pallas as pl
from jax.experimental.pallas import tpu as pltpu
from jax.sharding import PartitionSpec as P

HEADS = 6
LANES = 128
SUBLANES = 8


norm_floor = 0.25
masked_score = -1e30


def layer_norm(stream, gain):
    average = jnp.mean(stream, axis=-1, keepdims=True)
    centred = stream - average
    spread = jnp.mean(centred * centred, axis=-1, keepdims=True)
    return centred * lax.rsqrt(spread + norm_floor) * gain


def softmax_rows(scores):
    largest = jnp.max(scores, axis=-1, keepdims=True)
    exponent = jnp.exp(scores - largest)
    return exponent / jnp.sum(exponent, axis=-1, keepdims=True)


def plain_body(
    cells, n_train, present, norm_gain, feat_qkv, feat_out, item_qkv, item_out, mlp_in, mlp_out
):
    row_dev, feature_count, model_width = cells.shape
    devices_row = lax.axis_size("row")
    total_rows = row_dev * devices_row
    feat_dev = feature_count // devices_row
    head_size = model_width // HEADS
    scale = 1.0 / math.sqrt(head_size)
    query_rows = min(512, total_rows)
    highest = lax.Precision.HIGHEST
    normed = layer_norm(cells, norm_gain[0]).astype(jnp.bfloat16)
    triplet = jnp.einsum("rfe,ced->crfd", normed, feat_qkv, preferred_element_type=jnp.float32)
    triplet = triplet.reshape(3, row_dev, feature_count, HEADS, head_size)
    feat_values = triplet[2].astype(jnp.bfloat16)
    scores = jnp.einsum("rfhd,rghd->rhfg", triplet[0], triplet[1], precision=highest) * scale
    scores = jnp.where(present[None, None, None, :] > 0, scores, masked_score)
    weights = softmax_rows(scores).astype(jnp.bfloat16)
    context = jnp.einsum(
        "rhfg,rghd->rfhd", weights, feat_values, preferred_element_type=jnp.float32
    ).astype(jnp.bfloat16)
    context = context.reshape(row_dev, feature_count, model_width)
    cells_mid = cells + jnp.dot(context, feat_out, preferred_element_type=jnp.float32)
    key_live = lax.iota(jnp.int32, total_rows) < n_train[0]
    arrived = lax.all_to_all(
        cells_mid.reshape(row_dev, devices_row, feat_dev, model_width).astype(jnp.bfloat16),
        "row",
        split_axis=1,
        concat_axis=0,
        tiled=True,
    ).astype(jnp.float32)
    members = arrived.shape[2]
    stream = arrived.reshape(total_rows, members, model_width)
    normed_rows = layer_norm(stream, norm_gain[1]).astype(jnp.bfloat16)
    triples = jnp.einsum("rke,ced->kcrd", normed_rows, item_qkv, preferred_element_type=jnp.float32)

    def one_feature(triple):
        keys = triple[1].reshape(total_rows, HEADS, head_size)
        values = triple[2].astype(jnp.bfloat16).reshape(total_rows, HEADS, head_size)
        queries = triple[0].reshape(total_rows // query_rows, query_rows, HEADS, head_size)

        def query_group(chosen):
            group_scores = jnp.einsum("qhd,shd->hqs", chosen, keys, precision=highest) * scale
            group_scores = jnp.where(key_live[None, None, :], group_scores, masked_score)
            group_weights = softmax_rows(group_scores).astype(jnp.bfloat16)
            return jnp.einsum(
                "hqs,shd->qhd", group_weights, values, preferred_element_type=jnp.float32
            ).astype(jnp.bfloat16)

        return lax.map(query_group, queries).reshape(total_rows, model_width)

    gathered = lax.map(one_feature, triples)
    late = stream + jnp.dot(
        jnp.transpose(gathered, (1, 0, 2)), item_out, preferred_element_type=jnp.float32
    )
    normed_late = layer_norm(late, norm_gain[2]).astype(jnp.bfloat16)
    hidden = jax.nn.gelu(
        jnp.dot(normed_late, mlp_in, preferred_element_type=jnp.float32), approximate=False
    ).astype(jnp.bfloat16)
    updated = late + jnp.dot(hidden, mlp_out, preferred_element_type=jnp.float32)
    returned = lax.all_to_all(
        updated.reshape(total_rows, 1, members, model_width).astype(jnp.bfloat16),
        "row",
        split_axis=0,
        concat_axis=1,
        tiled=True,
    ).astype(jnp.float32)
    return returned.reshape(row_dev, feature_count, model_width)


def matmul(left, right, dims=(1, 0)):
    return lax.dot_general(
        left, right, (((dims[0],), (dims[1],)), ((), ())), preferred_element_type=jnp.float32
    )


def identity(size):
    down = lax.broadcasted_iota(jnp.int32, (size, size), 0)
    across = lax.broadcasted_iota(jnp.int32, (size, size), 1)
    return jnp.where(down == across, 1.0, 0.0).astype(jnp.bfloat16)


def prepare_weights(qkv_ref, turned_ref, spread_ref):
    width = qkv_ref.shape[1]
    head = width // HEADS
    eye = identity(width)
    turned_ref[:width, :] = matmul(eye, qkv_ref[0], (1, 1)).astype(jnp.bfloat16)
    turned_ref[width:, :] = matmul(eye, qkv_ref[2], (1, 1)).astype(jnp.bfloat16)
    down = lax.broadcasted_iota(jnp.int32, (width, 4 * width), 0)
    across = lax.broadcasted_iota(jnp.int32, (width, 4 * width), 1)
    source = (across // (4 * head)) * head + across % head
    pick = jnp.where(down == source, 1.0, 0.0).astype(jnp.bfloat16)
    spread_ref[...] = matmul(qkv_ref[1], pick).astype(jnp.bfloat16)


def attention(normed, turned_ref, spread_ref, bias_ref):
    tokens, width = normed.shape
    size = bias_ref.shape[0]
    head = width // HEADS
    wide = 4 * head
    turned = matmul(turned_ref[...], normed, (1, 1))
    keys = matmul(normed, spread_ref[...])
    queries = turned[:width] * (math.log2(math.e) / math.sqrt(head))
    query_high = queries.astype(jnp.bfloat16)
    query_low = (queries - query_high.astype(jnp.float32)).astype(jnp.bfloat16)
    values = turned[width:].astype(jnp.bfloat16)
    lane = lax.broadcasted_iota(jnp.int32, (1, 4 * width), 1)
    rounded = keys.astype(jnp.bfloat16).astype(jnp.float32)
    keys = jnp.where(lane % wide < 2 * head, keys, keys - rounded).astype(jnp.bfloat16)
    blocks = []
    for block in range(tokens // size):
        here = slice(block * size, (block + 1) * size)
        contexts = []
        for h in range(HEADS):
            rows = slice(h * head, (h + 1) * head)
            high, low = query_high[rows, here], query_low[rows, here]
            query = jnp.concatenate([high, low, high, low], axis=0)
            scores = matmul(keys[here, h * wide : (h + 1) * wide], query) + bias_ref[...]
            exponent = jnp.exp2(scores - jnp.max(scores, axis=0, keepdims=True))
            share = 1.0 / jnp.sum(exponent, axis=0, keepdims=True)
            weights = (exponent * share).astype(jnp.bfloat16)
            contexts.append(matmul(values[rows, here], weights))
        blocks.append(jnp.concatenate(contexts, axis=0))
    return blocks


def kernel(
    devices,
    n_train_ref, cells_ref, present_ref, gain_ref, feat_qkv_ref, feat_out_ref, item_qkv_ref,
    item_out_ref, mlp_in_ref, mlp_out_ref,
    out_ref,
    turned_f, spread_f, turned_i, spread_i, bias_f, bias_i, mid_a, mid_b, mid, send, recv, back,
    home, send_sem, recv_sem, back_sem, home_sem,
):
    me = lax.axis_index("row")
    rows, feats, width = cells_ref.shape
    feat_dev = feats // devices
    pairs = feat_dev // 2
    total_rows = rows * devices
    block = 2 * rows
    group = devices * block
    rest = width - LANES
    quarter = devices // 4
    order = list(range(2 * quarter, devices)) + list(range(quarter, 2 * quarter))
    order += list(range(1, quarter))

    def pack(slots, pair, tokens):
        last = tokens[:, LANES:].reshape(devices, 2, rows, rest)
        last = jnp.concatenate([last[:, 0], last[:, 1]], axis=-1)
        slots[pair, :, :block] = tokens[:, :LANES].reshape(devices, block, LANES).astype(jnp.bfloat16)
        slots[pair, :, block:] = last.astype(jnp.bfloat16)

    def unpack(slots, pair):
        first = slots[pair, :, :block].astype(jnp.float32).reshape(devices, 2, rows, LANES)
        last = slots[pair, :, block:].astype(jnp.float32)
        last = jnp.concatenate(
            [last[:, None, :, one * rest : (one + 1) * rest] for one in range(2)], axis=1
        )
        return jnp.concatenate([first, last], axis=-1)

    barrier = pltpu.get_barrier_semaphore()

    def greet(step, carry):
        pl.semaphore_signal(
            barrier, inc=1, device_id={"row": lax.rem(me + step, devices)},
            device_id_type=pl.DeviceIdType.MESH,
        )
        return carry

    lax.fori_loop(1, devices, greet, 0)

    prepare_weights(feat_qkv_ref, turned_f, spread_f)
    prepare_weights(item_qkv_ref, turned_i, spread_i)
    live = jnp.where(present_ref[...] > 0, 0.0, masked_score)
    bias_f[...] = jnp.broadcast_to(live, (feats, feats)).T
    number = lax.broadcasted_iota(jnp.int32, (total_rows, total_rows), 0)
    bias_i[...] = jnp.where(number < n_train_ref[0], 0.0, masked_score)

    def feature_rows(step, carry):
        cells = cells_ref[pl.ds(step * 2, 2)].reshape(2 * feats, width)
        normed = layer_norm(cells, gain_ref[0:1, :]).astype(jnp.bfloat16)
        contexts = attention(normed, turned_f, spread_f, bias_f)
        context = jnp.concatenate(contexts, axis=1).astype(jnp.bfloat16)
        updated = cells + matmul(context, feat_out_ref[...], (0, 0))
        here = pl.ds(pl.multiple_of(step * 2 * feats, 2 * feats), 2 * feats)
        mid_a[here, :] = updated[:, :LANES]
        mid_b[here, :rest] = updated[:, LANES:]
        return carry

    lax.fori_loop(0, rows // 2, feature_rows, 0)

    def outgoing(pair, step):
        to = lax.rem(me + step, devices)
        return pltpu.make_async_remote_copy(
            src_ref=send.at[pair, to], dst_ref=recv.at[pair, me],
            send_sem=send_sem.at[pair, step], recv_sem=recv_sem.at[pair, step],
            device_id={"row": to}, device_id_type=pl.DeviceIdType.MESH,
        )

    def returning(pair, step):
        to = lax.rem(me + step, devices)
        return pltpu.make_async_remote_copy(
            src_ref=back.at[pair, to], dst_ref=home.at[pair, me],
            send_sem=back_sem.at[pair, step], recv_sem=home_sem.at[pair, step],
            device_id={"row": to}, device_id_type=pl.DeviceIdType.MESH,
        )

    def each(act):
        def one(step, carry):
            act(step)
            return carry

        lax.fori_loop(1, devices, one, 0)

    pl.semaphore_wait(barrier, devices - 1)

    for pair in range(pairs):
        firsts, lasts = [], []
        for owner in range(devices):
            for one in range(2):
                take = pl.ds(owner * feat_dev + pair * 2 + one, rows, stride=feats)
                firsts.append(mid_a[take, :])
                lasts.append(mid_b[take, :])
        stream = jnp.concatenate(
            [jnp.concatenate(firsts, axis=0), jnp.concatenate(lasts, axis=0)[:, :rest]], axis=1
        )
        mid[pair] = stream
        normed = layer_norm(stream, gain_ref[1:2, :])
        pack(send, pair, normed)
        recv[pair, me] = send[pair, me]
        for step in order:
            outgoing(pair, step).start()

    def item_pair(pair, carry):
        each(lambda step: outgoing(pair, step).wait_recv())
        arrived = unpack(recv, pair)
        normed = jnp.concatenate(
            [arrived[:, one].reshape(total_rows, width) for one in range(2)], axis=0
        ).astype(jnp.bfloat16)
        contexts = attention(normed, turned_i, spread_i, bias_i)
        first = jnp.concatenate(
            [c[:LANES].T.reshape(devices, 1, rows, LANES) for c in contexts], axis=1
        )
        last = jnp.concatenate([c[LANES:] for c in contexts], axis=0).T
        back[pair, :, :block] = first.reshape(devices, block, LANES).astype(jnp.bfloat16)
        back[pair, :, block:] = last.reshape(devices, rows, LANES).astype(jnp.bfloat16)
        home[pair, me] = back[pair, me]
        for step in order:
            returning(pair, step).start()
        return carry

    lax.fori_loop(0, pairs, item_pair, 0)

    def finish(pair, carry):
        each(lambda step: returning(pair, step).wait_recv())
        context = unpack(home, pair).reshape(group, width).astype(jnp.bfloat16)
        late = mid[pair] + matmul(context, item_out_ref[...])
        normed = layer_norm(late, gain_ref[2:3, :]).astype(jnp.bfloat16)
        inner = matmul(normed, mlp_in_ref[...])
        hidden = (0.5 * inner * (1.0 + lax.erf(inner * math.sqrt(0.5)))).astype(jnp.bfloat16)
        done = late + matmul(hidden, mlp_out_ref[...], (1, 1))
        for owner in range(devices):
            for one in range(2):
                start = (owner * 2 + one) * rows
                put = pl.ds(owner * feat_dev + pair * 2 + one, rows, stride=feats)
                mid_a[put, :] = done[start : start + rows, :LANES]
                mid_b[put, :rest] = done[start : start + rows, LANES:]
        return carry

    lax.fori_loop(0, pairs, finish, 0)
    for row in range(rows):
        out_ref[row, :, :LANES] = mid_a[row * feats : (row + 1) * feats, :]
        out_ref[row, :, LANES:] = mid_b[row * feats : (row + 1) * feats, :rest]

    for pair in range(pairs):
        each(lambda step: outgoing(pair, step).wait_send())
        each(lambda step: returning(pair, step).wait_send())


def body(
    cells, n_train, present, norm_gain, feat_qkv, feat_out, item_qkv, item_out, mlp_in, mlp_out
):
    devices = lax.axis_size("row")
    rows, feats, width = cells.shape
    feat_dev = feats // devices
    fits = rows == SUBLANES and devices % 4 == 0 and feat_dev % 2 == 0 and 2 * width == 3 * LANES
    fits = fits and rows * devices == LANES and feats == LANES and width % (HEADS * 16) == 0
    if not fits:
        return plain_body(
            cells, n_train, present, norm_gain, feat_qkv, feat_out, item_qkv, item_out, mlp_in,
            mlp_out,
        )
    total_rows = rows * devices
    pairs = feat_dev // 2
    vmem = pl.BlockSpec(memory_space=pltpu.VMEM)
    bf16, f32 = jnp.bfloat16, jnp.float32
    slots = pltpu.VMEM((pairs, devices, 3 * rows, LANES), bf16)
    sems = pltpu.SemaphoreType.DMA((pairs, devices))
    return pl.pallas_call(
        functools.partial(kernel, devices),
        out_shape=jax.ShapeDtypeStruct(cells.shape, f32),
        in_specs=[pl.BlockSpec(memory_space=pltpu.SMEM)] + [vmem] * 9,
        out_specs=vmem,
        scratch_shapes=[
            pltpu.VMEM((2 * width, width), bf16),
            pltpu.VMEM((width, 4 * width), bf16),
            pltpu.VMEM((2 * width, width), bf16),
            pltpu.VMEM((width, 4 * width), bf16),
            pltpu.VMEM((feats, feats), f32),
            pltpu.VMEM((total_rows, total_rows), f32),
            pltpu.VMEM((rows * feats, LANES), f32),
            pltpu.VMEM((rows * feats, LANES), f32),
            pltpu.VMEM((pairs, 2 * total_rows, width), f32),
            slots, slots, slots, slots, sems, sems, sems, sems,
        ],
        compiler_params=pltpu.CompilerParams(
            collective_id=0, has_side_effects=True, vmem_limit_bytes=48 * 1024 * 1024
        ),
    )(
        n_train, cells, present.reshape(1, feats), norm_gain, feat_qkv, feat_out, item_qkv, item_out,
        mlp_in, mlp_out.T,
    )


def solution(mesh):
    return jax.shard_map(
        body,
        mesh=mesh,
        in_specs=(
            P(("grp", "row"), None, None),
            P("grp"),
            P("grp"),
            P(),
            P(),
            P(),
            P(),
            P(),
            P(),
            P(),
        ),
        out_specs=P(("grp", "row"), None, None),
        check_vma=False,
    )
```

```python
import functools
import math

import jax
import jax.numpy as jnp
from jax import lax
from jax.experimental import pallas as pl
from jax.experimental.pallas import tpu as pltpu
from jax.sharding import PartitionSpec as P

HEADS = 6
LANES = 128
SUBLANES = 8


norm_floor = 0.25
masked_score = -1e30


def layer_norm(stream, gain):
    average = jnp.mean(stream, axis=-1, keepdims=True)
    centred = stream - average
    spread = jnp.mean(centred * centred, axis=-1, keepdims=True)
    return centred * lax.rsqrt(spread + norm_floor) * gain


def softmax_rows(scores):
    largest = jnp.max(scores, axis=-1, keepdims=True)
    exponent = jnp.exp(scores - largest)
    return exponent / jnp.sum(exponent, axis=-1, keepdims=True)


def plain_body(
    cells, n_train, present, norm_gain, feat_qkv, feat_out, item_qkv, item_out, mlp_in, mlp_out
):
    row_dev, feature_count, model_width = cells.shape
    devices_row = lax.axis_size("row")
    total_rows = row_dev * devices_row
    feat_dev = feature_count // devices_row
    head_size = model_width // HEADS
    scale = 1.0 / math.sqrt(head_size)
    query_rows = min(512, total_rows)
    highest = lax.Precision.HIGHEST
    normed = layer_norm(cells, norm_gain[0]).astype(jnp.bfloat16)
    triplet = jnp.einsum("rfe,ced->crfd", normed, feat_qkv, preferred_element_type=jnp.float32)
    triplet = triplet.reshape(3, row_dev, feature_count, HEADS, head_size)
    feat_values = triplet[2].astype(jnp.bfloat16)
    scores = jnp.einsum("rfhd,rghd->rhfg", triplet[0], triplet[1], precision=highest) * scale
    scores = jnp.where(present[None, None, None, :] > 0, scores, masked_score)
    weights = softmax_rows(scores).astype(jnp.bfloat16)
    context = jnp.einsum(
        "rhfg,rghd->rfhd", weights, feat_values, preferred_element_type=jnp.float32
    ).astype(jnp.bfloat16)
    context = context.reshape(row_dev, feature_count, model_width)
    cells_mid = cells + jnp.dot(context, feat_out, preferred_element_type=jnp.float32)
    key_live = lax.iota(jnp.int32, total_rows) < n_train[0]
    arrived = lax.all_to_all(
        cells_mid.reshape(row_dev, devices_row, feat_dev, model_width).astype(jnp.bfloat16),
        "row",
        split_axis=1,
        concat_axis=0,
        tiled=True,
    ).astype(jnp.float32)
    members = arrived.shape[2]
    stream = arrived.reshape(total_rows, members, model_width)
    normed_rows = layer_norm(stream, norm_gain[1]).astype(jnp.bfloat16)
    triples = jnp.einsum("rke,ced->kcrd", normed_rows, item_qkv, preferred_element_type=jnp.float32)

    def one_feature(triple):
        keys = triple[1].reshape(total_rows, HEADS, head_size)
        values = triple[2].astype(jnp.bfloat16).reshape(total_rows, HEADS, head_size)
        queries = triple[0].reshape(total_rows // query_rows, query_rows, HEADS, head_size)

        def query_group(chosen):
            group_scores = jnp.einsum("qhd,shd->hqs", chosen, keys, precision=highest) * scale
            group_scores = jnp.where(key_live[None, None, :], group_scores, masked_score)
            group_weights = softmax_rows(group_scores).astype(jnp.bfloat16)
            return jnp.einsum(
                "hqs,shd->qhd", group_weights, values, preferred_element_type=jnp.float32
            ).astype(jnp.bfloat16)

        return lax.map(query_group, queries).reshape(total_rows, model_width)

    gathered = lax.map(one_feature, triples)
    late = stream + jnp.dot(
        jnp.transpose(gathered, (1, 0, 2)), item_out, preferred_element_type=jnp.float32
    )
    normed_late = layer_norm(late, norm_gain[2]).astype(jnp.bfloat16)
    hidden = jax.nn.gelu(
        jnp.dot(normed_late, mlp_in, preferred_element_type=jnp.float32), approximate=False
    ).astype(jnp.bfloat16)
    updated = late + jnp.dot(hidden, mlp_out, preferred_element_type=jnp.float32)
    returned = lax.all_to_all(
        updated.reshape(total_rows, 1, members, model_width).astype(jnp.bfloat16),
        "row",
        split_axis=0,
        concat_axis=1,
        tiled=True,
    ).astype(jnp.float32)
    return returned.reshape(row_dev, feature_count, model_width)


def matmul(left, right, dims=(1, 0)):
    return lax.dot_general(
        left, right, (((dims[0],), (dims[1],)), ((), ())), preferred_element_type=jnp.float32
    )


def identity(size):
    down = lax.broadcasted_iota(jnp.int32, (size, size), 0)
    across = lax.broadcasted_iota(jnp.int32, (size, size), 1)
    return jnp.where(down == across, 1.0, 0.0).astype(jnp.bfloat16)


def prepare_weights(qkv_ref, turned_ref, spread_ref):
    width = qkv_ref.shape[1]
    head = width // HEADS
    eye = identity(width)
    turned_ref[:width, :] = matmul(eye, qkv_ref[0], (1, 1)).astype(jnp.bfloat16)
    turned_ref[width:, :] = matmul(eye, qkv_ref[2], (1, 1)).astype(jnp.bfloat16)
    down = lax.broadcasted_iota(jnp.int32, (width, 4 * width), 0)
    across = lax.broadcasted_iota(jnp.int32, (width, 4 * width), 1)
    source = (across // (4 * head)) * head + across % head
    pick = jnp.where(down == source, 1.0, 0.0).astype(jnp.bfloat16)
    spread_ref[...] = matmul(qkv_ref[1], pick).astype(jnp.bfloat16)


def attention(normed, turned_ref, spread_ref, bias_ref):
    tokens, width = normed.shape
    size = bias_ref.shape[0]
    head = width // HEADS
    wide = 4 * head
    turned = matmul(turned_ref[...], normed, (1, 1))
    keys = matmul(normed, spread_ref[...])
    queries = turned[:width] * (math.log2(math.e) / math.sqrt(head))
    query_high = queries.astype(jnp.bfloat16)
    query_low = (queries - query_high.astype(jnp.float32)).astype(jnp.bfloat16)
    values = turned[width:].astype(jnp.bfloat16)
    lane = lax.broadcasted_iota(jnp.int32, (1, 4 * width), 1)
    rounded = keys.astype(jnp.bfloat16).astype(jnp.float32)
    keys = jnp.where(lane % wide < 2 * head, keys, keys - rounded).astype(jnp.bfloat16)
    blocks = []
    for block in range(tokens // size):
        here = slice(block * size, (block + 1) * size)
        contexts = []
        for h in range(HEADS):
            rows = slice(h * head, (h + 1) * head)
            high, low = query_high[rows, here], query_low[rows, here]
            query = jnp.concatenate([high, low, high, low], axis=0)
            scores = matmul(keys[here, h * wide : (h + 1) * wide], query) + bias_ref[...]
            exponent = jnp.exp2(scores - jnp.max(scores, axis=0, keepdims=True))
            share = 1.0 / jnp.sum(exponent, axis=0, keepdims=True)
            weights = (exponent * share).astype(jnp.bfloat16)
            contexts.append(matmul(values[rows, here], weights))
        blocks.append(jnp.concatenate(contexts, axis=0))
    return blocks


def kernel(
    devices,
    n_train_ref, cells_ref, present_ref, gain_ref, feat_qkv_ref, feat_out_ref, item_qkv_ref,
    item_out_ref, mlp_in_ref, mlp_out_ref,
    out_ref,
    turned_f, spread_f, turned_i, spread_i, bias_f, bias_i, mid_a, mid_b, mid, send, recv, back,
    home, send_sem, recv_sem, back_sem, home_sem,
):
    me = lax.axis_index("row")
    rows, width, feats = cells_ref.shape
    feat_dev = feats // devices
    pairs = feat_dev // 2
    total_rows = rows * devices
    block = 2 * rows
    group = devices * block
    rest = width - LANES
    order = range(1, devices)

    def pack(slots, pair, tokens):
        last = tokens[:, LANES:].reshape(devices, 2, rows, rest)
        last = jnp.concatenate([last[:, 0], last[:, 1]], axis=-1)
        slots[pair, :, :block] = tokens[:, :LANES].reshape(devices, block, LANES).astype(jnp.bfloat16)
        slots[pair, :, block:] = last.astype(jnp.bfloat16)

    def unpack(slots, pair):
        first = slots[pair, :, :block].astype(jnp.float32).reshape(devices, 2, rows, LANES)
        last = slots[pair, :, block:].astype(jnp.float32)
        last = jnp.concatenate(
            [last[:, None, :, one * rest : (one + 1) * rest] for one in range(2)], axis=1
        )
        return jnp.concatenate([first, last], axis=-1)

    barrier = pltpu.get_barrier_semaphore()

    def greet(step, carry):
        pl.semaphore_signal(
            barrier, inc=1, device_id={"row": lax.rem(me + step, devices)},
            device_id_type=pl.DeviceIdType.MESH,
        )
        return carry

    lax.fori_loop(1, devices, greet, 0)

    prepare_weights(feat_qkv_ref, turned_f, spread_f)
    prepare_weights(item_qkv_ref, turned_i, spread_i)
    live = jnp.where(present_ref[...] > 0, 0.0, masked_score)
    bias_f[...] = jnp.broadcast_to(live, (feats, feats)).T
    number = lax.broadcasted_iota(jnp.int32, (total_rows, total_rows), 0)
    bias_i[...] = jnp.where(number < n_train_ref[0], 0.0, masked_score)

    def feature_rows(step, carry):
        cells = jnp.concatenate([cells_ref[step * 2 + one].T for one in range(2)], axis=0)
        normed = layer_norm(cells, gain_ref[0:1, :]).astype(jnp.bfloat16)
        contexts = attention(normed, turned_f, spread_f, bias_f)
        context = jnp.concatenate(contexts, axis=1).astype(jnp.bfloat16)
        updated = cells + matmul(context, feat_out_ref[...], (0, 0))
        here = pl.ds(pl.multiple_of(step * 2 * feats, 2 * feats), 2 * feats)
        mid_a[here, :] = updated[:, :LANES]
        mid_b[here, :rest] = updated[:, LANES:]
        return carry

    lax.fori_loop(0, rows // 2, feature_rows, 0)

    def outgoing(pair, step):
        to = lax.rem(me + step, devices)
        return pltpu.make_async_remote_copy(
            src_ref=send.at[pair, to], dst_ref=recv.at[pair, me],
            send_sem=send_sem.at[pair, step], recv_sem=recv_sem.at[pair, step],
            device_id={"row": to}, device_id_type=pl.DeviceIdType.MESH,
        )

    def returning(pair, step):
        to = lax.rem(me + step, devices)
        return pltpu.make_async_remote_copy(
            src_ref=back.at[pair, to], dst_ref=home.at[pair, me],
            send_sem=back_sem.at[pair, step], recv_sem=home_sem.at[pair, step],
            device_id={"row": to}, device_id_type=pl.DeviceIdType.MESH,
        )

    def each(act):
        def one(step, carry):
            act(step)
            return carry

        lax.fori_loop(1, devices, one, 0)

    pl.semaphore_wait(barrier, devices - 1)

    for pair in range(pairs):
        firsts, lasts = [], []
        for owner in range(devices):
            for one in range(2):
                take = pl.ds(owner * feat_dev + pair * 2 + one, rows, stride=feats)
                firsts.append(mid_a[take, :])
                lasts.append(mid_b[take, :])
        stream = jnp.concatenate(
            [jnp.concatenate(firsts, axis=0), jnp.concatenate(lasts, axis=0)[:, :rest]], axis=1
        )
        mid[pair] = stream
        normed = layer_norm(stream, gain_ref[1:2, :])
        pack(send, pair, normed)
        recv[pair, me] = send[pair, me]
        for step in order:
            outgoing(pair, step).start()

    def item_pair(pair, carry):
        each(lambda step: outgoing(pair, step).wait_recv())
        arrived = unpack(recv, pair)
        normed = jnp.concatenate(
            [arrived[:, one].reshape(total_rows, width) for one in range(2)], axis=0
        ).astype(jnp.bfloat16)
        contexts = attention(normed, turned_i, spread_i, bias_i)
        first = jnp.concatenate(
            [c[:LANES].T.reshape(devices, 1, rows, LANES) for c in contexts], axis=1
        )
        last = jnp.concatenate([c[LANES:] for c in contexts], axis=0).T
        back[pair, :, :block] = first.reshape(devices, block, LANES).astype(jnp.bfloat16)
        back[pair, :, block:] = last.reshape(devices, rows, LANES).astype(jnp.bfloat16)
        home[pair, me] = back[pair, me]
        for step in order:
            returning(pair, step).start()
        return carry

    lax.fori_loop(0, pairs, item_pair, 0)

    def finish(pair, carry):
        each(lambda step: returning(pair, step).wait_recv())
        context = unpack(home, pair).reshape(group, width).astype(jnp.bfloat16)
        late = mid[pair] + matmul(context, item_out_ref[...])
        normed = layer_norm(late, gain_ref[2:3, :]).astype(jnp.bfloat16)
        inner = matmul(normed, mlp_in_ref[...])
        hidden = (0.5 * inner * (1.0 + lax.erf(inner * math.sqrt(0.5)))).astype(jnp.bfloat16)
        done = late + matmul(hidden, mlp_out_ref[...], (1, 1))
        for owner in range(devices):
            for one in range(2):
                start = (owner * 2 + one) * rows
                put = pl.ds(owner * feat_dev + pair * 2 + one, rows, stride=feats)
                mid_a[put, :] = done[start : start + rows, :LANES]
                mid_b[put, :rest] = done[start : start + rows, LANES:]
        return carry

    lax.fori_loop(0, pairs, finish, 0)
    for row in range(rows):
        out_ref[row, :, :LANES] = mid_a[row * feats : (row + 1) * feats, :]
        out_ref[row, :, LANES:] = mid_b[row * feats : (row + 1) * feats, :rest]

    for pair in range(pairs):
        each(lambda step: outgoing(pair, step).wait_send())
        each(lambda step: returning(pair, step).wait_send())


def body(
    cells, n_train, present, norm_gain, feat_qkv, feat_out, item_qkv, item_out, mlp_in, mlp_out
):
    devices = lax.axis_size("row")
    rows, feats, width = cells.shape
    feat_dev = feats // devices
    fits = rows == SUBLANES and feat_dev % 2 == 0 and 2 * width == 3 * LANES
    fits = fits and rows * devices == LANES and feats == LANES and width % (HEADS * 16) == 0
    if not fits:
        return plain_body(
            cells, n_train, present, norm_gain, feat_qkv, feat_out, item_qkv, item_out, mlp_in,
            mlp_out,
        )
    total_rows = rows * devices
    pairs = feat_dev // 2
    vmem = pl.BlockSpec(memory_space=pltpu.VMEM)
    bf16, f32 = jnp.bfloat16, jnp.float32
    slots = pltpu.VMEM((pairs, devices, 3 * rows, LANES), bf16)
    sems = pltpu.SemaphoreType.DMA((pairs, devices))
    return pl.pallas_call(
        functools.partial(kernel, devices),
        out_shape=jax.ShapeDtypeStruct(cells.shape, f32),
        in_specs=[pl.BlockSpec(memory_space=pltpu.SMEM)] + [vmem] * 9,
        out_specs=vmem,
        scratch_shapes=[
            pltpu.VMEM((2 * width, width), bf16),
            pltpu.VMEM((width, 4 * width), bf16),
            pltpu.VMEM((2 * width, width), bf16),
            pltpu.VMEM((width, 4 * width), bf16),
            pltpu.VMEM((feats, feats), f32),
            pltpu.VMEM((total_rows, total_rows), f32),
            pltpu.VMEM((rows * feats, LANES), f32),
            pltpu.VMEM((rows * feats, LANES), f32),
            pltpu.VMEM((pairs, 2 * total_rows, width), f32),
            slots, slots, slots, slots, sems, sems, sems, sems,
        ],
        compiler_params=pltpu.CompilerParams(
            collective_id=0, has_side_effects=True, vmem_limit_bytes=48 * 1024 * 1024
        ),
    )(
        n_train, jnp.transpose(cells, (0, 2, 1)), present.reshape(1, feats), norm_gain, feat_qkv, feat_out, item_qkv, item_out,
        mlp_in, mlp_out.T,
    )


def solution(mesh):
    return jax.shard_map(
        body,
        mesh=mesh,
        in_specs=(
            P(("grp", "row"), None, None),
            P("grp"),
            P("grp"),
            P(),
            P(),
            P(),
            P(),
            P(),
            P(),
            P(),
        ),
        out_specs=P(("grp", "row"), None, None),
        check_vma=False,
    )
```

```python
import functools
import math

import jax
import jax.numpy as jnp
from jax import lax
from jax.experimental import pallas as pl
from jax.experimental.pallas import tpu as pltpu
from jax.sharding import PartitionSpec as P

HEADS = 6
LANES = 128
SUBLANES = 8


norm_floor = 0.25
masked_score = -1e30


def layer_norm(stream, gain):
    average = jnp.mean(stream, axis=-1, keepdims=True)
    centred = stream - average
    spread = jnp.mean(centred * centred, axis=-1, keepdims=True)
    return centred * lax.rsqrt(spread + norm_floor) * gain


def softmax_rows(scores):
    largest = jnp.max(scores, axis=-1, keepdims=True)
    exponent = jnp.exp(scores - largest)
    return exponent / jnp.sum(exponent, axis=-1, keepdims=True)


def plain_body(
    cells, n_train, present, norm_gain, feat_qkv, feat_out, item_qkv, item_out, mlp_in, mlp_out
):
    row_dev, feature_count, model_width = cells.shape
    devices_row = lax.axis_size("row")
    total_rows = row_dev * devices_row
    feat_dev = feature_count // devices_row
    head_size = model_width // HEADS
    scale = 1.0 / math.sqrt(head_size)
    query_rows = min(512, total_rows)
    highest = lax.Precision.HIGHEST
    normed = layer_norm(cells, norm_gain[0]).astype(jnp.bfloat16)
    triplet = jnp.einsum("rfe,ced->crfd", normed, feat_qkv, preferred_element_type=jnp.float32)
    triplet = triplet.reshape(3, row_dev, feature_count, HEADS, head_size)
    feat_values = triplet[2].astype(jnp.bfloat16)
    scores = jnp.einsum("rfhd,rghd->rhfg", triplet[0], triplet[1], precision=highest) * scale
    scores = jnp.where(present[None, None, None, :] > 0, scores, masked_score)
    weights = softmax_rows(scores).astype(jnp.bfloat16)
    context = jnp.einsum(
        "rhfg,rghd->rfhd", weights, feat_values, preferred_element_type=jnp.float32
    ).astype(jnp.bfloat16)
    context = context.reshape(row_dev, feature_count, model_width)
    cells_mid = cells + jnp.dot(context, feat_out, preferred_element_type=jnp.float32)
    key_live = lax.iota(jnp.int32, total_rows) < n_train[0]
    arrived = lax.all_to_all(
        cells_mid.reshape(row_dev, devices_row, feat_dev, model_width).astype(jnp.bfloat16),
        "row",
        split_axis=1,
        concat_axis=0,
        tiled=True,
    ).astype(jnp.float32)
    members = arrived.shape[2]
    stream = arrived.reshape(total_rows, members, model_width)
    normed_rows = layer_norm(stream, norm_gain[1]).astype(jnp.bfloat16)
    triples = jnp.einsum("rke,ced->kcrd", normed_rows, item_qkv, preferred_element_type=jnp.float32)

    def one_feature(triple):
        keys = triple[1].reshape(total_rows, HEADS, head_size)
        values = triple[2].astype(jnp.bfloat16).reshape(total_rows, HEADS, head_size)
        queries = triple[0].reshape(total_rows // query_rows, query_rows, HEADS, head_size)

        def query_group(chosen):
            group_scores = jnp.einsum("qhd,shd->hqs", chosen, keys, precision=highest) * scale
            group_scores = jnp.where(key_live[None, None, :], group_scores, masked_score)
            group_weights = softmax_rows(group_scores).astype(jnp.bfloat16)
            return jnp.einsum(
                "hqs,shd->qhd", group_weights, values, preferred_element_type=jnp.float32
            ).astype(jnp.bfloat16)

        return lax.map(query_group, queries).reshape(total_rows, model_width)

    gathered = lax.map(one_feature, triples)
    late = stream + jnp.dot(
        jnp.transpose(gathered, (1, 0, 2)), item_out, preferred_element_type=jnp.float32
    )
    normed_late = layer_norm(late, norm_gain[2]).astype(jnp.bfloat16)
    hidden = jax.nn.gelu(
        jnp.dot(normed_late, mlp_in, preferred_element_type=jnp.float32), approximate=False
    ).astype(jnp.bfloat16)
    updated = late + jnp.dot(hidden, mlp_out, preferred_element_type=jnp.float32)
    returned = lax.all_to_all(
        updated.reshape(total_rows, 1, members, model_width).astype(jnp.bfloat16),
        "row",
        split_axis=0,
        concat_axis=1,
        tiled=True,
    ).astype(jnp.float32)
    return returned.reshape(row_dev, feature_count, model_width)


def matmul(left, right, dims=(1, 0)):
    return lax.dot_general(
        left, right, (((dims[0],), (dims[1],)), ((), ())), preferred_element_type=jnp.float32
    )


def identity(size):
    down = lax.broadcasted_iota(jnp.int32, (size, size), 0)
    across = lax.broadcasted_iota(jnp.int32, (size, size), 1)
    return jnp.where(down == across, 1.0, 0.0).astype(jnp.bfloat16)


def prepare_weights(qkv_ref, turned_ref, spread_ref):
    width = qkv_ref.shape[1]
    head = width // HEADS
    eye = identity(width)
    turned_ref[:width, :] = matmul(eye, qkv_ref[0], (1, 1)).astype(jnp.bfloat16)
    turned_ref[width:, :] = matmul(eye, qkv_ref[2], (1, 1)).astype(jnp.bfloat16)
    down = lax.broadcasted_iota(jnp.int32, (width, 4 * width), 0)
    across = lax.broadcasted_iota(jnp.int32, (width, 4 * width), 1)
    source = (across // (4 * head)) * head + across % head
    pick = jnp.where(down == source, 1.0, 0.0).astype(jnp.bfloat16)
    spread_ref[...] = matmul(qkv_ref[1], pick).astype(jnp.bfloat16)


def attention(normed, turned_ref, spread_ref, bias_ref):
    tokens, width = normed.shape
    size = bias_ref.shape[0]
    head = width // HEADS
    wide = 4 * head
    turned = matmul(turned_ref[...], normed, (1, 1))
    keys = matmul(normed, spread_ref[...])
    queries = turned[:width] * (math.log2(math.e) / math.sqrt(head))
    query_high = queries.astype(jnp.bfloat16)
    query_low = (queries - query_high.astype(jnp.float32)).astype(jnp.bfloat16)
    values = turned[width:].astype(jnp.bfloat16)
    lane = lax.broadcasted_iota(jnp.int32, (1, 4 * width), 1)
    rounded = keys.astype(jnp.bfloat16).astype(jnp.float32)
    keys = jnp.where(lane % wide < 2 * head, keys, keys - rounded).astype(jnp.bfloat16)
    blocks = []
    for block in range(tokens // size):
        here = slice(block * size, (block + 1) * size)
        contexts = []
        for h in range(HEADS):
            rows = slice(h * head, (h + 1) * head)
            high, low = query_high[rows, here], query_low[rows, here]
            query = jnp.concatenate([high, low, high, low], axis=0)
            scores = matmul(keys[here, h * wide : (h + 1) * wide], query) + bias_ref[...]
            exponent = jnp.exp2(scores - jnp.max(scores, axis=0, keepdims=True))
            share = 1.0 / jnp.sum(exponent, axis=0, keepdims=True)
            weights = (exponent * share).astype(jnp.bfloat16)
            contexts.append(matmul(values[rows, here], weights))
        blocks.append(jnp.concatenate(contexts, axis=0))
    return blocks


def kernel(
    devices,
    n_train_ref, gain_ref, present_ref, feat_qkv_hbm, item_qkv_hbm, cells_hbm, feat_out_hbm,
    item_out_hbm, mlp_in_hbm, mlp_out_hbm,
    out_ref,
    feat_qkv_ref, item_qkv_ref, cells_ref, feat_out_ref, item_out_ref, mlp_in_ref, mlp_out_ref,
    load_sem,
    turned_f, spread_f, turned_i, spread_i, bias_f, bias_i, mid_a, mid_b, mid, send, recv, back,
    home, send_sem, recv_sem, back_sem, home_sem,
):
    me = lax.axis_index("row")
    rows, width, feats = cells_ref.shape
    feat_dev = feats // devices
    pairs = feat_dev // 2
    total_rows = rows * devices
    block = 2 * rows
    group = devices * block
    rest = width - LANES
    order = range(1, devices)

    def pack(slots, pair, tokens):
        last = tokens[:, LANES:].reshape(devices, 2, rows, rest)
        last = jnp.concatenate([last[:, 0], last[:, 1]], axis=-1)
        slots[pair, :, :block] = tokens[:, :LANES].reshape(devices, block, LANES).astype(jnp.bfloat16)
        slots[pair, :, block:] = last.astype(jnp.bfloat16)

    def unpack(slots, pair):
        first = slots[pair, :, :block].astype(jnp.float32).reshape(devices, 2, rows, LANES)
        last = slots[pair, :, block:].astype(jnp.float32)
        last = jnp.concatenate(
            [last[:, None, :, one * rest : (one + 1) * rest] for one in range(2)], axis=1
        )
        return jnp.concatenate([first, last], axis=-1)

    loads = [
        pltpu.make_async_copy(source, target, load_sem.at[number])
        for number, (source, target) in enumerate((
            (feat_qkv_hbm, feat_qkv_ref), (item_qkv_hbm, item_qkv_ref), (cells_hbm, cells_ref),
            (feat_out_hbm, feat_out_ref), (item_out_hbm, item_out_ref), (mlp_in_hbm, mlp_in_ref),
            (mlp_out_hbm, mlp_out_ref),
        ))
    ]
    for load in loads:
        load.start()
    barrier = pltpu.get_barrier_semaphore()

    def greet(step, carry):
        pl.semaphore_signal(
            barrier, inc=1, device_id={"row": lax.rem(me + step, devices)},
            device_id_type=pl.DeviceIdType.MESH,
        )
        return carry

    lax.fori_loop(1, devices, greet, 0)

    loads[0].wait()
    prepare_weights(feat_qkv_ref, turned_f, spread_f)
    loads[1].wait()
    prepare_weights(item_qkv_ref, turned_i, spread_i)
    live = jnp.where(present_ref[...] > 0, 0.0, masked_score)
    bias_f[...] = jnp.broadcast_to(live, (feats, feats)).T
    number = lax.broadcasted_iota(jnp.int32, (total_rows, total_rows), 0)
    bias_i[...] = jnp.where(number < n_train_ref[0], 0.0, masked_score)

    loads[2].wait()
    loads[3].wait()

    def feature_rows(step, carry):
        cells = jnp.concatenate([cells_ref[step * 2 + one].T for one in range(2)], axis=0)
        normed = layer_norm(cells, gain_ref[0:1, :]).astype(jnp.bfloat16)
        contexts = attention(normed, turned_f, spread_f, bias_f)
        context = jnp.concatenate(contexts, axis=1).astype(jnp.bfloat16)
        updated = cells + matmul(context, feat_out_ref[...], (0, 0))
        here = pl.ds(pl.multiple_of(step * 2 * feats, 2 * feats), 2 * feats)
        mid_a[here, :] = updated[:, :LANES]
        mid_b[here, :rest] = updated[:, LANES:]
        return carry

    lax.fori_loop(0, rows // 2, feature_rows, 0)

    def outgoing(pair, step):
        to = lax.rem(me + step, devices)
        return pltpu.make_async_remote_copy(
            src_ref=send.at[pair, to], dst_ref=recv.at[pair, me],
            send_sem=send_sem.at[pair, step], recv_sem=recv_sem.at[pair, step],
            device_id={"row": to}, device_id_type=pl.DeviceIdType.MESH,
        )

    def returning(pair, step):
        to = lax.rem(me + step, devices)
        return pltpu.make_async_remote_copy(
            src_ref=back.at[pair, to], dst_ref=home.at[pair, me],
            send_sem=back_sem.at[pair, step], recv_sem=home_sem.at[pair, step],
            device_id={"row": to}, device_id_type=pl.DeviceIdType.MESH,
        )

    def each(act):
        def one(step, carry):
            act(step)
            return carry

        lax.fori_loop(1, devices, one, 0)

    pl.semaphore_wait(barrier, devices - 1)

    for pair in range(pairs):
        firsts, lasts = [], []
        for owner in range(devices):
            for one in range(2):
                take = pl.ds(owner * feat_dev + pair * 2 + one, rows, stride=feats)
                firsts.append(mid_a[take, :])
                lasts.append(mid_b[take, :])
        stream = jnp.concatenate(
            [jnp.concatenate(firsts, axis=0), jnp.concatenate(lasts, axis=0)[:, :rest]], axis=1
        )
        mid[pair] = stream
        normed = layer_norm(stream, gain_ref[1:2, :])
        pack(send, pair, normed)
        recv[pair, me] = send[pair, me]
        for step in order:
            outgoing(pair, step).start()

    def item_pair(pair, carry):
        each(lambda step: outgoing(pair, step).wait_recv())
        arrived = unpack(recv, pair)
        normed = jnp.concatenate(
            [arrived[:, one].reshape(total_rows, width) for one in range(2)], axis=0
        ).astype(jnp.bfloat16)
        contexts = attention(normed, turned_i, spread_i, bias_i)
        first = jnp.concatenate(
            [c[:LANES].T.reshape(devices, 1, rows, LANES) for c in contexts], axis=1
        )
        last = jnp.concatenate([c[LANES:] for c in contexts], axis=0).T
        back[pair, :, :block] = first.reshape(devices, block, LANES).astype(jnp.bfloat16)
        back[pair, :, block:] = last.reshape(devices, rows, LANES).astype(jnp.bfloat16)
        home[pair, me] = back[pair, me]
        for step in order:
            returning(pair, step).start()
        return carry

    lax.fori_loop(0, pairs, item_pair, 0)

    for load in loads[4:]:
        load.wait()

    def finish(pair, carry):
        each(lambda step: returning(pair, step).wait_recv())
        context = unpack(home, pair).reshape(group, width).astype(jnp.bfloat16)
        late = mid[pair] + matmul(context, item_out_ref[...])
        normed = layer_norm(late, gain_ref[2:3, :]).astype(jnp.bfloat16)
        inner = matmul(normed, mlp_in_ref[...])
        hidden = (0.5 * inner * (1.0 + lax.erf(inner * math.sqrt(0.5)))).astype(jnp.bfloat16)
        done = late + matmul(hidden, mlp_out_ref[...], (1, 1))
        for owner in range(devices):
            for one in range(2):
                start = (owner * 2 + one) * rows
                put = pl.ds(owner * feat_dev + pair * 2 + one, rows, stride=feats)
                mid_a[put, :] = done[start : start + rows, :LANES]
                mid_b[put, :rest] = done[start : start + rows, LANES:]
        return carry

    lax.fori_loop(0, pairs, finish, 0)
    for row in range(rows):
        out_ref[row, :, :LANES] = mid_a[row * feats : (row + 1) * feats, :]
        out_ref[row, :, LANES:] = mid_b[row * feats : (row + 1) * feats, :rest]

    for pair in range(pairs):
        each(lambda step: outgoing(pair, step).wait_send())
        each(lambda step: returning(pair, step).wait_send())


def body(
    cells, n_train, present, norm_gain, feat_qkv, feat_out, item_qkv, item_out, mlp_in, mlp_out
):
    devices = lax.axis_size("row")
    rows, feats, width = cells.shape
    feat_dev = feats // devices
    fits = rows == SUBLANES and feat_dev % 2 == 0 and 2 * width == 3 * LANES
    fits = fits and rows * devices == LANES and feats == LANES and width % (HEADS * 16) == 0
    if not fits:
        return plain_body(
            cells, n_train, present, norm_gain, feat_qkv, feat_out, item_qkv, item_out, mlp_in,
            mlp_out,
        )
    total_rows = rows * devices
    pairs = feat_dev // 2
    vmem = pl.BlockSpec(memory_space=pltpu.VMEM)
    bf16, f32 = jnp.bfloat16, jnp.float32
    slots = pltpu.VMEM((pairs, devices, 3 * rows, LANES), bf16)
    sems = pltpu.SemaphoreType.DMA((pairs, devices))
    arrays = (
        feat_qkv, item_qkv, jnp.transpose(cells, (0, 2, 1)), feat_out, item_out, mlp_in, mlp_out.T,
    )
    return pl.pallas_call(
        functools.partial(kernel, devices),
        out_shape=jax.ShapeDtypeStruct(cells.shape, f32),
        in_specs=[pl.BlockSpec(memory_space=pltpu.SMEM), vmem, vmem]
        + [pl.BlockSpec(memory_space=pltpu.HBM)] * 7,
        out_specs=vmem,
        scratch_shapes=[pltpu.VMEM(array.shape, array.dtype) for array in arrays]
        + [
            pltpu.SemaphoreType.DMA((len(arrays),)),
            pltpu.VMEM((2 * width, width), bf16),
            pltpu.VMEM((width, 4 * width), bf16),
            pltpu.VMEM((2 * width, width), bf16),
            pltpu.VMEM((width, 4 * width), bf16),
            pltpu.VMEM((feats, feats), f32),
            pltpu.VMEM((total_rows, total_rows), f32),
            pltpu.VMEM((rows * feats, LANES), f32),
            pltpu.VMEM((rows * feats, LANES), f32),
            pltpu.VMEM((pairs, 2 * total_rows, width), f32),
            slots, slots, slots, slots, sems, sems, sems, sems,
        ],
        compiler_params=pltpu.CompilerParams(
            collective_id=0, has_side_effects=True, vmem_limit_bytes=62 * 1024 * 1024 + 512 * 1024
        ),
    )(
        n_train, norm_gain, present.reshape(1, feats), *arrays
    )


def solution(mesh):
    return jax.shard_map(
        body,
        mesh=mesh,
        in_specs=(
            P(("grp", "row"), None, None),
            P("grp"),
            P("grp"),
            P(),
            P(),
            P(),
            P(),
            P(),
            P(),
            P(),
        ),
        out_specs=P(("grp", "row"), None, None),
        check_vma=False,
    )
```

```python
import functools
import math

import jax
import jax.numpy as jnp
from jax import lax
from jax.experimental import pallas as pl
from jax.experimental.pallas import tpu as pltpu
from jax.sharding import PartitionSpec as P

HEADS = 6
LANES = 128
SUBLANES = 8


norm_floor = 0.25
masked_score = -1e30


def layer_norm(stream, gain):
    average = jnp.mean(stream, axis=-1, keepdims=True)
    centred = stream - average
    spread = jnp.mean(centred * centred, axis=-1, keepdims=True)
    return centred * lax.rsqrt(spread + norm_floor) * gain


def softmax_rows(scores):
    largest = jnp.max(scores, axis=-1, keepdims=True)
    exponent = jnp.exp(scores - largest)
    return exponent / jnp.sum(exponent, axis=-1, keepdims=True)


def plain_body(
    cells, n_train, present, norm_gain, feat_qkv, feat_out, item_qkv, item_out, mlp_in, mlp_out
):
    row_dev, feature_count, model_width = cells.shape
    devices_row = lax.axis_size("row")
    total_rows = row_dev * devices_row
    feat_dev = feature_count // devices_row
    head_size = model_width // HEADS
    scale = 1.0 / math.sqrt(head_size)
    query_rows = min(512, total_rows)
    highest = lax.Precision.HIGHEST
    normed = layer_norm(cells, norm_gain[0]).astype(jnp.bfloat16)
    triplet = jnp.einsum("rfe,ced->crfd", normed, feat_qkv, preferred_element_type=jnp.float32)
    triplet = triplet.reshape(3, row_dev, feature_count, HEADS, head_size)
    feat_values = triplet[2].astype(jnp.bfloat16)
    scores = jnp.einsum("rfhd,rghd->rhfg", triplet[0], triplet[1], precision=highest) * scale
    scores = jnp.where(present[None, None, None, :] > 0, scores, masked_score)
    weights = softmax_rows(scores).astype(jnp.bfloat16)
    context = jnp.einsum(
        "rhfg,rghd->rfhd", weights, feat_values, preferred_element_type=jnp.float32
    ).astype(jnp.bfloat16)
    context = context.reshape(row_dev, feature_count, model_width)
    cells_mid = cells + jnp.dot(context, feat_out, preferred_element_type=jnp.float32)
    key_live = lax.iota(jnp.int32, total_rows) < n_train[0]
    arrived = lax.all_to_all(
        cells_mid.reshape(row_dev, devices_row, feat_dev, model_width).astype(jnp.bfloat16),
        "row",
        split_axis=1,
        concat_axis=0,
        tiled=True,
    ).astype(jnp.float32)
    members = arrived.shape[2]
    stream = arrived.reshape(total_rows, members, model_width)
    normed_rows = layer_norm(stream, norm_gain[1]).astype(jnp.bfloat16)
    triples = jnp.einsum("rke,ced->kcrd", normed_rows, item_qkv, preferred_element_type=jnp.float32)

    def one_feature(triple):
        keys = triple[1].reshape(total_rows, HEADS, head_size)
        values = triple[2].astype(jnp.bfloat16).reshape(total_rows, HEADS, head_size)
        queries = triple[0].reshape(total_rows // query_rows, query_rows, HEADS, head_size)

        def query_group(chosen):
            group_scores = jnp.einsum("qhd,shd->hqs", chosen, keys, precision=highest) * scale
            group_scores = jnp.where(key_live[None, None, :], group_scores, masked_score)
            group_weights = softmax_rows(group_scores).astype(jnp.bfloat16)
            return jnp.einsum(
                "hqs,shd->qhd", group_weights, values, preferred_element_type=jnp.float32
            ).astype(jnp.bfloat16)

        return lax.map(query_group, queries).reshape(total_rows, model_width)

    gathered = lax.map(one_feature, triples)
    late = stream + jnp.dot(
        jnp.transpose(gathered, (1, 0, 2)), item_out, preferred_element_type=jnp.float32
    )
    normed_late = layer_norm(late, norm_gain[2]).astype(jnp.bfloat16)
    hidden = jax.nn.gelu(
        jnp.dot(normed_late, mlp_in, preferred_element_type=jnp.float32), approximate=False
    ).astype(jnp.bfloat16)
    updated = late + jnp.dot(hidden, mlp_out, preferred_element_type=jnp.float32)
    returned = lax.all_to_all(
        updated.reshape(total_rows, 1, members, model_width).astype(jnp.bfloat16),
        "row",
        split_axis=0,
        concat_axis=1,
        tiled=True,
    ).astype(jnp.float32)
    return returned.reshape(row_dev, feature_count, model_width)


def matmul(left, right, dims=(1, 0)):
    return lax.dot_general(
        left, right, (((dims[0],), (dims[1],)), ((), ())), preferred_element_type=jnp.float32
    )


def identity(size):
    down = lax.broadcasted_iota(jnp.int32, (size, size), 0)
    across = lax.broadcasted_iota(jnp.int32, (size, size), 1)
    return jnp.where(down == across, 1.0, 0.0).astype(jnp.bfloat16)


def prepare_weights(qkv_ref, turned_ref, spread_ref):
    width = qkv_ref.shape[1]
    head = width // HEADS
    eye = identity(width)
    turned_ref[:width, :] = matmul(eye, qkv_ref[0], (1, 1)).astype(jnp.bfloat16)
    turned_ref[width:, :] = matmul(eye, qkv_ref[2], (1, 1)).astype(jnp.bfloat16)
    down = lax.broadcasted_iota(jnp.int32, (width, 4 * width), 0)
    across = lax.broadcasted_iota(jnp.int32, (width, 4 * width), 1)
    source = (across // (4 * head)) * head + across % head
    pick = jnp.where(down == source, 1.0, 0.0).astype(jnp.bfloat16)
    spread_ref[...] = matmul(qkv_ref[1], pick).astype(jnp.bfloat16)


def attention(normed, turned_ref, spread_ref, bias_ref):
    tokens, width = normed.shape
    size = bias_ref.shape[0]
    head = width // HEADS
    wide = 4 * head
    turned = matmul(turned_ref[...], normed, (1, 1))
    keys = matmul(normed, spread_ref[...])
    queries = turned[:width] * (math.log2(math.e) / math.sqrt(head))
    query_high = queries.astype(jnp.bfloat16)
    query_low = (queries - query_high.astype(jnp.float32)).astype(jnp.bfloat16)
    values = turned[width:].astype(jnp.bfloat16)
    lane = lax.broadcasted_iota(jnp.int32, (1, 4 * width), 1)
    rounded = keys.astype(jnp.bfloat16).astype(jnp.float32)
    keys = jnp.where(lane % wide < 2 * head, keys, keys - rounded).astype(jnp.bfloat16)
    blocks = []
    for block in range(tokens // size):
        here = slice(block * size, (block + 1) * size)
        contexts = []
        for h in range(HEADS):
            rows = slice(h * head, (h + 1) * head)
            high, low = query_high[rows, here], query_low[rows, here]
            query = jnp.concatenate([high, low, high, low], axis=0)
            scores = matmul(keys[here, h * wide : (h + 1) * wide], query) + bias_ref[...]
            exponent = jnp.exp2(scores - jnp.max(scores, axis=0, keepdims=True))
            share = 1.0 / jnp.sum(exponent, axis=0, keepdims=True)
            weights = (exponent * share).astype(jnp.bfloat16)
            contexts.append(matmul(values[rows, here], weights))
        blocks.append(jnp.concatenate(contexts, axis=0))
    return blocks


def kernel(
    devices,
    n_train_ref, cells_ref, present_ref, gain_ref, feat_qkv_ref, feat_out_ref, item_qkv_ref,
    item_out_ref, mlp_in_ref, mlp_out_ref,
    out_ref,
    turned_f, spread_f, turned_i, spread_i, bias_f, bias_i, mid_a, mid_b, mid, send, recv, back,
    home, send_sem, recv_sem, back_sem, home_sem,
):
    me = lax.axis_index("row")
    rows, feats, width = cells_ref.shape
    feat_dev = feats // devices
    pairs = feat_dev // 2
    total_rows = rows * devices
    block = 2 * rows
    group = devices * block
    rest = width - LANES
    order = range(1, devices)

    def pack(slots, pair, tokens):
        last = tokens[:, LANES:].reshape(devices, 2, rows, rest)
        last = jnp.concatenate([last[:, 0], last[:, 1]], axis=-1)
        slots[pair, :, :block] = tokens[:, :LANES].reshape(devices, block, LANES).astype(jnp.bfloat16)
        slots[pair, :, block:] = last.astype(jnp.bfloat16)

    def unpack(slots, pair):
        first = slots[pair, :, :block].astype(jnp.float32).reshape(devices, 2, rows, LANES)
        last = slots[pair, :, block:].astype(jnp.float32)
        last = jnp.concatenate(
            [last[:, None, :, one * rest : (one + 1) * rest] for one in range(2)], axis=1
        )
        return jnp.concatenate([first, last], axis=-1)

    barrier = pltpu.get_barrier_semaphore()

    def greet(step, carry):
        pl.semaphore_signal(
            barrier, inc=1, device_id={"row": lax.rem(me + step, devices)},
            device_id_type=pl.DeviceIdType.MESH,
        )
        return carry

    lax.fori_loop(1, devices, greet, 0)

    prepare_weights(feat_qkv_ref, turned_f, spread_f)
    live = jnp.where(present_ref[...] > 0, 0.0, masked_score)
    bias_f[...] = jnp.broadcast_to(live, (feats, feats)).T
    def feature_rows(step, carry):
        cells = cells_ref[pl.ds(step * 2, 2)].reshape(2 * feats, width)
        normed = layer_norm(cells, gain_ref[0:1, :]).astype(jnp.bfloat16)
        contexts = attention(normed, turned_f, spread_f, bias_f)
        context = jnp.concatenate(contexts, axis=1).astype(jnp.bfloat16)
        updated = cells + matmul(context, feat_out_ref[...], (0, 0))
        here = pl.ds(pl.multiple_of(step * 2 * feats, 2 * feats), 2 * feats)
        mid_a[here, :] = updated[:, :LANES]
        mid_b[here, :rest] = updated[:, LANES:]
        return carry

    lax.fori_loop(0, rows // 2, feature_rows, 0)

    def outgoing(pair, step):
        to = lax.rem(me + step, devices)
        return pltpu.make_async_remote_copy(
            src_ref=send.at[pair, to], dst_ref=recv.at[pair, me],
            send_sem=send_sem.at[pair, step], recv_sem=recv_sem.at[pair, step],
            device_id={"row": to}, device_id_type=pl.DeviceIdType.MESH,
        )

    def returning(pair, step):
        to = lax.rem(me + step, devices)
        return pltpu.make_async_remote_copy(
            src_ref=back.at[pair, to], dst_ref=home.at[pair, me],
            send_sem=back_sem.at[pair, step], recv_sem=home_sem.at[pair, step],
            device_id={"row": to}, device_id_type=pl.DeviceIdType.MESH,
        )

    def each(act):
        def one(step, carry):
            act(step)
            return carry

        lax.fori_loop(1, devices, one, 0)

    pl.semaphore_wait(barrier, devices - 1)

    for pair in range(pairs):
        firsts, lasts = [], []
        for owner in range(devices):
            for one in range(2):
                take = pl.ds(owner * feat_dev + pair * 2 + one, rows, stride=feats)
                firsts.append(mid_a[take, :])
                lasts.append(mid_b[take, :])
        stream = jnp.concatenate(
            [jnp.concatenate(firsts, axis=0), jnp.concatenate(lasts, axis=0)[:, :rest]], axis=1
        )
        mid[pair] = stream
        normed = layer_norm(stream, gain_ref[1:2, :])
        pack(send, pair, normed)
        recv[pair, me] = send[pair, me]
        for step in order:
            outgoing(pair, step).start()

    prepare_weights(item_qkv_ref, turned_i, spread_i)
    number = lax.broadcasted_iota(jnp.int32, (total_rows, total_rows), 0)
    bias_i[...] = jnp.where(number < n_train_ref[0], 0.0, masked_score)

    def item_pair(pair, carry):
        each(lambda step: outgoing(pair, step).wait_recv())
        arrived = unpack(recv, pair)
        normed = jnp.concatenate(
            [arrived[:, one].reshape(total_rows, width) for one in range(2)], axis=0
        ).astype(jnp.bfloat16)
        contexts = attention(normed, turned_i, spread_i, bias_i)
        first = jnp.concatenate(
            [c[:LANES].T.reshape(devices, 1, rows, LANES) for c in contexts], axis=1
        )
        last = jnp.concatenate([c[LANES:] for c in contexts], axis=0).T
        back[pair, :, :block] = first.reshape(devices, block, LANES).astype(jnp.bfloat16)
        back[pair, :, block:] = last.reshape(devices, rows, LANES).astype(jnp.bfloat16)
        home[pair, me] = back[pair, me]
        for step in order:
            returning(pair, step).start()
        each(lambda step: outgoing(pair, step).wait_send())
        return carry

    lax.fori_loop(0, pairs, item_pair, 0)

    def finish(pair, carry):
        each(lambda step: returning(pair, step).wait_send())
        each(lambda step: returning(pair, step).wait_recv())
        context = unpack(home, pair).reshape(group, width).astype(jnp.bfloat16)
        late = mid[pair] + matmul(context, item_out_ref[...])
        normed = layer_norm(late, gain_ref[2:3, :]).astype(jnp.bfloat16)
        inner = matmul(normed, mlp_in_ref[...])
        hidden = (0.5 * inner * (1.0 + lax.erf(inner * math.sqrt(0.5)))).astype(jnp.bfloat16)
        done = late + matmul(hidden, mlp_out_ref[...], (1, 1))
        for owner in range(devices):
            for one in range(2):
                start = (owner * 2 + one) * rows
                put = pl.ds(owner * feat_dev + pair * 2 + one, rows, stride=feats)
                mid_a[put, :] = done[start : start + rows, :LANES]
                mid_b[put, :rest] = done[start : start + rows, LANES:]
        return carry

    lax.fori_loop(0, pairs, finish, 0)
    for row in range(rows):
        out_ref[row, :, :LANES] = mid_a[row * feats : (row + 1) * feats, :]
        out_ref[row, :, LANES:] = mid_b[row * feats : (row + 1) * feats, :rest]


def body(
    cells, n_train, present, norm_gain, feat_qkv, feat_out, item_qkv, item_out, mlp_in, mlp_out
):
    devices = lax.axis_size("row")
    rows, feats, width = cells.shape
    feat_dev = feats // devices
    fits = rows == SUBLANES and feat_dev % 2 == 0 and 2 * width == 3 * LANES
    fits = fits and rows * devices == LANES and feats == LANES and width % (HEADS * 16) == 0
    if not fits:
        return plain_body(
            cells, n_train, present, norm_gain, feat_qkv, feat_out, item_qkv, item_out, mlp_in,
            mlp_out,
        )
    total_rows = rows * devices
    pairs = feat_dev // 2
    vmem = pl.BlockSpec(memory_space=pltpu.VMEM)
    bf16, f32 = jnp.bfloat16, jnp.float32
    slots = pltpu.VMEM((pairs, devices, 3 * rows, LANES), bf16)
    sems = pltpu.SemaphoreType.DMA((pairs, devices))
    return pl.pallas_call(
        functools.partial(kernel, devices),
        out_shape=jax.ShapeDtypeStruct(cells.shape, f32),
        in_specs=[pl.BlockSpec(memory_space=pltpu.SMEM)] + [vmem] * 9,
        out_specs=vmem,
        scratch_shapes=[
            pltpu.VMEM((2 * width, width), bf16),
            pltpu.VMEM((width, 4 * width), bf16),
            pltpu.VMEM((2 * width, width), bf16),
            pltpu.VMEM((width, 4 * width), bf16),
            pltpu.VMEM((feats, feats), f32),
            pltpu.VMEM((total_rows, total_rows), f32),
            pltpu.VMEM((rows * feats, LANES), f32),
            pltpu.VMEM((rows * feats, LANES), f32),
            pltpu.VMEM((pairs, 2 * total_rows, width), f32),
            slots, slots, slots, slots, sems, sems, sems, sems,
        ],
        compiler_params=pltpu.CompilerParams(
            collective_id=0, has_side_effects=True, vmem_limit_bytes=48 * 1024 * 1024
        ),
    )(
        n_train, cells, present.reshape(1, feats), norm_gain, feat_qkv, feat_out, item_qkv, item_out,
        mlp_in, mlp_out.T,
    )


def solution(mesh):
    return jax.shard_map(
        body,
        mesh=mesh,
        in_specs=(
            P(("grp", "row"), None, None),
            P("grp"),
            P("grp"),
            P(),
            P(),
            P(),
            P(),
            P(),
            P(),
            P(),
        ),
        out_specs=P(("grp", "row"), None, None),
        check_vma=False,
    )
```

```python
import functools
import math

import jax
import jax.numpy as jnp
from jax import lax
from jax.experimental import pallas as pl
from jax.experimental.pallas import tpu as pltpu
from jax.sharding import PartitionSpec as P

HEADS = 6
LANES = 128
SUBLANES = 8


norm_floor = 0.25
masked_score = -1e30


def layer_norm(stream, gain):
    average = jnp.mean(stream, axis=-1, keepdims=True)
    centred = stream - average
    spread = jnp.mean(centred * centred, axis=-1, keepdims=True)
    return centred * lax.rsqrt(spread + norm_floor) * gain


def softmax_rows(scores):
    largest = jnp.max(scores, axis=-1, keepdims=True)
    exponent = jnp.exp(scores - largest)
    return exponent / jnp.sum(exponent, axis=-1, keepdims=True)


def plain_body(
    cells, n_train, present, norm_gain, feat_qkv, feat_out, item_qkv, item_out, mlp_in, mlp_out
):
    row_dev, feature_count, model_width = cells.shape
    devices_row = lax.axis_size("row")
    total_rows = row_dev * devices_row
    feat_dev = feature_count // devices_row
    head_size = model_width // HEADS
    scale = 1.0 / math.sqrt(head_size)
    query_rows = min(512, total_rows)
    highest = lax.Precision.HIGHEST
    normed = layer_norm(cells, norm_gain[0]).astype(jnp.bfloat16)
    triplet = jnp.einsum("rfe,ced->crfd", normed, feat_qkv, preferred_element_type=jnp.float32)
    triplet = triplet.reshape(3, row_dev, feature_count, HEADS, head_size)
    feat_values = triplet[2].astype(jnp.bfloat16)
    scores = jnp.einsum("rfhd,rghd->rhfg", triplet[0], triplet[1], precision=highest) * scale
    scores = jnp.where(present[None, None, None, :] > 0, scores, masked_score)
    weights = softmax_rows(scores).astype(jnp.bfloat16)
    context = jnp.einsum(
        "rhfg,rghd->rfhd", weights, feat_values, preferred_element_type=jnp.float32
    ).astype(jnp.bfloat16)
    context = context.reshape(row_dev, feature_count, model_width)
    cells_mid = cells + jnp.dot(context, feat_out, preferred_element_type=jnp.float32)
    key_live = lax.iota(jnp.int32, total_rows) < n_train[0]
    arrived = lax.all_to_all(
        cells_mid.reshape(row_dev, devices_row, feat_dev, model_width).astype(jnp.bfloat16),
        "row",
        split_axis=1,
        concat_axis=0,
        tiled=True,
    ).astype(jnp.float32)
    members = arrived.shape[2]
    stream = arrived.reshape(total_rows, members, model_width)
    normed_rows = layer_norm(stream, norm_gain[1]).astype(jnp.bfloat16)
    triples = jnp.einsum("rke,ced->kcrd", normed_rows, item_qkv, preferred_element_type=jnp.float32)

    def one_feature(triple):
        keys = triple[1].reshape(total_rows, HEADS, head_size)
        values = triple[2].astype(jnp.bfloat16).reshape(total_rows, HEADS, head_size)
        queries = triple[0].reshape(total_rows // query_rows, query_rows, HEADS, head_size)

        def query_group(chosen):
            group_scores = jnp.einsum("qhd,shd->hqs", chosen, keys, precision=highest) * scale
            group_scores = jnp.where(key_live[None, None, :], group_scores, masked_score)
            group_weights = softmax_rows(group_scores).astype(jnp.bfloat16)
            return jnp.einsum(
                "hqs,shd->qhd", group_weights, values, preferred_element_type=jnp.float32
            ).astype(jnp.bfloat16)

        return lax.map(query_group, queries).reshape(total_rows, model_width)

    gathered = lax.map(one_feature, triples)
    late = stream + jnp.dot(
        jnp.transpose(gathered, (1, 0, 2)), item_out, preferred_element_type=jnp.float32
    )
    normed_late = layer_norm(late, norm_gain[2]).astype(jnp.bfloat16)
    hidden = jax.nn.gelu(
        jnp.dot(normed_late, mlp_in, preferred_element_type=jnp.float32), approximate=False
    ).astype(jnp.bfloat16)
    updated = late + jnp.dot(hidden, mlp_out, preferred_element_type=jnp.float32)
    returned = lax.all_to_all(
        updated.reshape(total_rows, 1, members, model_width).astype(jnp.bfloat16),
        "row",
        split_axis=0,
        concat_axis=1,
        tiled=True,
    ).astype(jnp.float32)
    return returned.reshape(row_dev, feature_count, model_width)


def matmul(left, right, dims=(1, 0)):
    return lax.dot_general(
        left, right, (((dims[0],), (dims[1],)), ((), ())), preferred_element_type=jnp.float32
    )


def identity(size):
    down = lax.broadcasted_iota(jnp.int32, (size, size), 0)
    across = lax.broadcasted_iota(jnp.int32, (size, size), 1)
    return jnp.where(down == across, 1.0, 0.0).astype(jnp.bfloat16)


def prepare_weights(qkv_ref, turned_ref, spread_ref):
    width = qkv_ref.shape[1]
    head = width // HEADS
    eye = identity(width)
    turned_ref[:width, :] = matmul(eye, qkv_ref[0], (1, 1)).astype(jnp.bfloat16)
    turned_ref[width:, :] = matmul(eye, qkv_ref[2], (1, 1)).astype(jnp.bfloat16)
    down = lax.broadcasted_iota(jnp.int32, (width, 4 * width), 0)
    across = lax.broadcasted_iota(jnp.int32, (width, 4 * width), 1)
    source = (across // (4 * head)) * head + across % head
    pick = jnp.where(down == source, 1.0, 0.0).astype(jnp.bfloat16)
    spread_ref[...] = matmul(qkv_ref[1], pick).astype(jnp.bfloat16)


def attention(normed, turned_ref, spread_ref, bias_ref):
    tokens, width = normed.shape
    size = bias_ref.shape[0]
    head = width // HEADS
    wide = 4 * head
    turned = matmul(turned_ref[...], normed, (1, 1))
    keys = matmul(normed, spread_ref[...])
    queries = turned[:width] * (math.log2(math.e) / math.sqrt(head))
    query_high = queries.astype(jnp.bfloat16)
    query_low = (queries - query_high.astype(jnp.float32)).astype(jnp.bfloat16)
    values = turned[width:].astype(jnp.bfloat16)
    lane = lax.broadcasted_iota(jnp.int32, (1, 4 * width), 1)
    rounded = keys.astype(jnp.bfloat16).astype(jnp.float32)
    keys = jnp.where(lane % wide < 2 * head, keys, keys - rounded).astype(jnp.bfloat16)
    blocks = []
    for block in range(tokens // size):
        here = slice(block * size, (block + 1) * size)
        contexts = []
        for h in range(HEADS):
            rows = slice(h * head, (h + 1) * head)
            high, low = query_high[rows, here], query_low[rows, here]
            query = jnp.concatenate([high, low, high, low], axis=0)
            scores = matmul(keys[here, h * wide : (h + 1) * wide], query) + bias_ref[...]
            exponent = jnp.exp2(scores - jnp.max(scores, axis=0, keepdims=True))
            share = 1.0 / jnp.sum(exponent, axis=0, keepdims=True)
            weights = (exponent * share).astype(jnp.bfloat16)
            contexts.append(matmul(values[rows, here], weights))
        blocks.append(jnp.concatenate(contexts, axis=0))
    return blocks


def kernel(
    devices,
    n_train_ref, cells_ref, present_ref, gain_ref, feat_qkv_ref, feat_out_ref, item_qkv_ref,
    item_out_ref, mlp_in_ref, mlp_out_ref,
    out_ref,
    turned_f, spread_f, turned_i, spread_i, bias_f, bias_i, mid_a, mid_b, mid, send, recv, back,
    home, send_sem, recv_sem, back_sem, home_sem,
):
    me = lax.axis_index("row")
    rows, feats, width = cells_ref.shape
    feat_dev = feats // devices
    pairs = feat_dev // 2
    total_rows = rows * devices
    block = 2 * rows
    group = devices * block
    rest = width - LANES
    order = range(1, devices)

    def pack(slots, pair, tokens):
        last = tokens[:, LANES:].reshape(devices, 2, rows, rest)
        last = jnp.concatenate([last[:, 0], last[:, 1]], axis=-1)
        slots[pair, :, :block] = tokens[:, :LANES].reshape(devices, block, LANES).astype(jnp.bfloat16)
        slots[pair, :, block:] = last.astype(jnp.bfloat16)

    def unpack(slots, pair):
        first = slots[pair, :, :block].astype(jnp.float32).reshape(devices, 2, rows, LANES)
        last = slots[pair, :, block:].astype(jnp.float32)
        last = jnp.concatenate(
            [last[:, None, :, one * rest : (one + 1) * rest] for one in range(2)], axis=1
        )
        return jnp.concatenate([first, last], axis=-1)

    barrier = pltpu.get_barrier_semaphore()

    def greet(step, carry):
        pl.semaphore_signal(
            barrier, inc=1, device_id={"row": lax.rem(me + step, devices)},
            device_id_type=pl.DeviceIdType.MESH,
        )
        return carry

    lax.fori_loop(1, devices, greet, 0)

    prepare_weights(feat_qkv_ref, turned_f, spread_f)
    live = jnp.where(present_ref[...] > 0, 0.0, masked_score)
    bias_f[...] = jnp.broadcast_to(live, (feats, feats)).T
    def feature_rows(step, carry):
        cells = cells_ref[pl.ds(step * 2, 2)].reshape(2 * feats, width)
        normed = layer_norm(cells, gain_ref[0:1, :]).astype(jnp.bfloat16)
        contexts = attention(normed, turned_f, spread_f, bias_f)
        context = jnp.concatenate(contexts, axis=1).astype(jnp.bfloat16)
        updated = cells + matmul(context, feat_out_ref[...], (0, 0))
        here = pl.ds(pl.multiple_of(step * 2 * feats, 2 * feats), 2 * feats)
        mid_a[here, :] = updated[:, :LANES]
        mid_b[here, :rest] = updated[:, LANES:]
        return carry

    lax.fori_loop(0, rows // 2, feature_rows, 0, unroll=2)

    def outgoing(pair, step):
        to = lax.rem(me + step, devices)
        return pltpu.make_async_remote_copy(
            src_ref=send.at[pair, to], dst_ref=recv.at[pair, me],
            send_sem=send_sem.at[pair, step], recv_sem=recv_sem.at[pair, step],
            device_id={"row": to}, device_id_type=pl.DeviceIdType.MESH,
        )

    def returning(pair, step):
        to = lax.rem(me + step, devices)
        return pltpu.make_async_remote_copy(
            src_ref=back.at[pair, to], dst_ref=home.at[pair, me],
            send_sem=back_sem.at[pair, step], recv_sem=home_sem.at[pair, step],
            device_id={"row": to}, device_id_type=pl.DeviceIdType.MESH,
        )

    def each(act):
        def one(step, carry):
            act(step)
            return carry

        lax.fori_loop(1, devices, one, 0)

    pl.semaphore_wait(barrier, devices - 1)

    for pair in range(pairs):
        firsts, lasts = [], []
        for owner in range(devices):
            for one in range(2):
                take = pl.ds(owner * feat_dev + pair * 2 + one, rows, stride=feats)
                firsts.append(mid_a[take, :])
                lasts.append(mid_b[take, :])
        stream = jnp.concatenate(
            [jnp.concatenate(firsts, axis=0), jnp.concatenate(lasts, axis=0)[:, :rest]], axis=1
        )
        mid[pair] = stream
        normed = layer_norm(stream, gain_ref[1:2, :])
        pack(send, pair, normed)
        recv[pair, me] = send[pair, me]
        for step in order:
            outgoing(pair, step).start()

    prepare_weights(item_qkv_ref, turned_i, spread_i)
    number = lax.broadcasted_iota(jnp.int32, (total_rows, total_rows), 0)
    bias_i[...] = jnp.where(number < n_train_ref[0], 0.0, masked_score)

    def item_pair(pair, carry):
        each(lambda step: outgoing(pair, step).wait_recv())
        arrived = unpack(recv, pair)
        normed = jnp.concatenate(
            [arrived[:, one].reshape(total_rows, width) for one in range(2)], axis=0
        ).astype(jnp.bfloat16)
        contexts = attention(normed, turned_i, spread_i, bias_i)
        first = jnp.concatenate(
            [c[:LANES].T.reshape(devices, 1, rows, LANES) for c in contexts], axis=1
        )
        last = jnp.concatenate([c[LANES:] for c in contexts], axis=0).T
        back[pair, :, :block] = first.reshape(devices, block, LANES).astype(jnp.bfloat16)
        back[pair, :, block:] = last.reshape(devices, rows, LANES).astype(jnp.bfloat16)
        home[pair, me] = back[pair, me]
        for step in order:
            returning(pair, step).start()
        each(lambda step: outgoing(pair, step).wait_send())
        return carry

    lax.fori_loop(0, pairs, item_pair, 0)

    def finish(pair, carry):
        each(lambda step: returning(pair, step).wait_send())
        each(lambda step: returning(pair, step).wait_recv())
        context = unpack(home, pair).reshape(group, width).astype(jnp.bfloat16)
        late = mid[pair] + matmul(context, item_out_ref[...])
        normed = layer_norm(late, gain_ref[2:3, :]).astype(jnp.bfloat16)
        inner = matmul(normed, mlp_in_ref[...])
        hidden = (0.5 * inner * (1.0 + lax.erf(inner * math.sqrt(0.5)))).astype(jnp.bfloat16)
        done = late + matmul(hidden, mlp_out_ref[...], (1, 1))
        for owner in range(devices):
            for one in range(2):
                start = (owner * 2 + one) * rows
                put = pl.ds(owner * feat_dev + pair * 2 + one, rows, stride=feats)
                mid_a[put, :] = done[start : start + rows, :LANES]
                mid_b[put, :rest] = done[start : start + rows, LANES:]
        return carry

    lax.fori_loop(0, pairs, finish, 0)
    for row in range(rows):
        out_ref[row, :, :LANES] = mid_a[row * feats : (row + 1) * feats, :]
        out_ref[row, :, LANES:] = mid_b[row * feats : (row + 1) * feats, :rest]


def body(
    cells, n_train, present, norm_gain, feat_qkv, feat_out, item_qkv, item_out, mlp_in, mlp_out
):
    devices = lax.axis_size("row")
    rows, feats, width = cells.shape
    feat_dev = feats // devices
    fits = rows == SUBLANES and feat_dev % 2 == 0 and 2 * width == 3 * LANES
    fits = fits and rows * devices == LANES and feats == LANES and width % (HEADS * 16) == 0
    if not fits:
        return plain_body(
            cells, n_train, present, norm_gain, feat_qkv, feat_out, item_qkv, item_out, mlp_in,
            mlp_out,
        )
    total_rows = rows * devices
    pairs = feat_dev // 2
    vmem = pl.BlockSpec(memory_space=pltpu.VMEM)
    bf16, f32 = jnp.bfloat16, jnp.float32
    slots = pltpu.VMEM((pairs, devices, 3 * rows, LANES), bf16)
    sems = pltpu.SemaphoreType.DMA((pairs, devices))
    return pl.pallas_call(
        functools.partial(kernel, devices),
        out_shape=jax.ShapeDtypeStruct(cells.shape, f32),
        in_specs=[pl.BlockSpec(memory_space=pltpu.SMEM)] + [vmem] * 9,
        out_specs=vmem,
        scratch_shapes=[
            pltpu.VMEM((2 * width, width), bf16),
            pltpu.VMEM((width, 4 * width), bf16),
            pltpu.VMEM((2 * width, width), bf16),
            pltpu.VMEM((width, 4 * width), bf16),
            pltpu.VMEM((feats, feats), f32),
            pltpu.VMEM((total_rows, total_rows), f32),
            pltpu.VMEM((rows * feats, LANES), f32),
            pltpu.VMEM((rows * feats, LANES), f32),
            pltpu.VMEM((pairs, 2 * total_rows, width), f32),
            slots, slots, slots, slots, sems, sems, sems, sems,
        ],
        compiler_params=pltpu.CompilerParams(
            collective_id=0, has_side_effects=True, vmem_limit_bytes=48 * 1024 * 1024
        ),
    )(
        n_train, cells, present.reshape(1, feats), norm_gain, feat_qkv, feat_out, item_qkv, item_out,
        mlp_in, mlp_out.T,
    )


def solution(mesh):
    return jax.shard_map(
        body,
        mesh=mesh,
        in_specs=(
            P(("grp", "row"), None, None),
            P("grp"),
            P("grp"),
            P(),
            P(),
            P(),
            P(),
            P(),
            P(),
            P(),
        ),
        out_specs=P(("grp", "row"), None, None),
        check_vma=False,
    )
```
